32 devices in a mesh: dp: 8 (over z, x), tensor: 4 (over y, core).
Axes of the slice: x: 2, y: 2, z: 4, core: 2. Of those that a mesh axis runs over, the one named last changes fastest.
Arguments:
- inputs: bfloat16 [16384, 768], P(('dp', 'tensor')), may hold values from -6 to 6
- out_grad: bfloat16 [16384, 768], P(('dp', 'tensor')), may hold values from -6 to 6
- offsets: int32 [32, 2], P('dp'), may hold values from 64 to 512, as said below
- key_keep: int32 [16384], P('dp'), may hold values 0 or 1
- project_weight: bfloat16 [768, 3, 768], P(None, None, 'tensor'), may hold values from -0.21875 to 0.21875
- project_bias: bfloat16 [2, 768], P(None, 'tensor'), may hold values from -3 to 3
- output_weight: bfloat16 [768, 768], P('tensor'), may hold values from -1.25 to 1.25
- output_bias: bfloat16 [2, 768], replicated, may hold values from -3 to 3
- norm_gains: bfloat16 [2, 768], replicated, may hold values from 0.099609375 to 1.8984375
- norm_shifts: bfloat16 [2, 768], replicated, may hold values from -3 to 3
- up_weight: bfloat16 [768, 3072], P(None, 'tensor'), may hold values from -0.21875 to 0.21875
- up_bias: bfloat16 [3072], P('tensor'), may hold values from -3 to 3
- down_weight: bfloat16 [3072, 768], P('tensor'), may hold values from -0.109375 to 0.109375
Outputs:
- layer_output: bfloat16 [16384, 768], P(('dp', 'tensor'))
- input_grad: bfloat16 [16384, 768], P(('dp', 'tensor'))
- project_weight_grad: float32 [768, 3, 768], P(None, None, 'tensor')
- project_bias_grad: float32 [2, 768], P(None, 'tensor')
- output_weight_grad: float32 [768, 768], P('tensor')
- output_bias_grad: float32 [2, 768], replicated
- norm_gains_grad: float32 [2, 768], replicated
- norm_shifts_grad: float32 [2, 768], replicated
- up_weight_grad: float32 [768, 3072], P(None, 'tensor')
- up_bias_grad: float32 [3072], P('tensor')
- down_weight_grad: float32 [3072, 768], P('tensor')
The draws below stay inside these ranges and needn't reach their ends.
Inputs may be any that keep to these rules, and one draw needn't show every extreme that they name: `offsets`: row s gives the end of slot s's passage and then the end of its query, which follows with 1 to 20 tokens; the rest of the slot up to 512 is padding. A passage has an eighth of 512 tokens or more. In every aligned block of 4 rows some slot ends at 512 and some passage has exactly an eighth of 512 tokens.
All inputs are finite; a program needn't handle non-finite values. No bound on the sum of `key_keep` on one device may be relied on, other than what follows from the above.
Results may differ from the reference program's by a relative error of at most 0.019.
The reference program's roundings to bfloat16 on the way count: a program that leaves them out, or rounds other values in their place, can miss the bound.
Values may be sent and summed in bfloat16 or wider, within the bound.
A program may use at most 128 MiB of HBM per device.

```python
import jax
import jax.numpy as jnp
from jax import lax

D = 768
HEADS = 12
HD = 64
FF = 3072
SLOT = 512
QLEN = 20
SEQ_DP = 4
SEQS = 32
TOKENS = 16384


def draw_offsets(key, part):
    key_one, key_two, key_three = jax.random.split(key, 3)
    query_len = jax.random.randint(key_one, (SEQS,), 1, QLEN + 1)
    passage = jax.random.randint(key_two, (SEQS,), SLOT // 8, SLOT - QLEN + 1)
    chosen_slot = jax.random.randint(key_three, (SEQS // SEQ_DP,), 0, SEQ_DP)
    slot_index = jnp.arange(SEQS) % SEQ_DP
    block_choice = chosen_slot[jnp.arange(SEQS) // SEQ_DP]
    full_slot = block_choice == slot_index
    short_slot = (block_choice + 1) % SEQ_DP == slot_index
    passage = jnp.where(short_slot, SLOT // 8, passage)
    passage = jnp.where(full_slot, SLOT - query_len, passage)
    return jnp.stack([passage, passage + query_len], axis=1).astype(jnp.int32)


def place_ends(result, rng, least, high):
    longest = result.shape.index(max(result.shape))
    spots = []
    for shift in (0, 1):
        where = [jax.random.randint(jax.random.fold_in(rng, axis), (), 0, length) for axis, length in enumerate(result.shape)]
        where[longest] = (where[longest] + shift) % result.shape[longest]
        spots.append(tuple(where))
    return result.at[spots[0]].set(least).at[spots[1]].set(high)


def level_of(own_key, dims, shards, low, high):
    level, own = 1.0, jax.random.fold_in(own_key, 6)
    for axis_at, shards_of in shards:
        heights = jnp.exp(jax.random.uniform(jax.random.fold_in(own, axis_at), (shards_of,), jnp.float32, low / len(shards), high / len(shards)))
        level = level * jnp.repeat(heights, dims[axis_at] // shards_of).reshape([-1 if axis == axis_at else 1 for axis in range(len(dims))])
    return level


def bell_draw(own_key, extent, width, limit, cuts=(), held_as=jnp.bfloat16):
    array = width * jax.random.normal(own_key, extent, jnp.float32)
    if cuts:
        array = array * level_of(own_key, extent, cuts, -0.22, 0.18)
    return jnp.clip(array, -limit, limit).astype(held_as)


def setup_inputs(seed: int = 0) -> dict:
    splits = jax.random.split(jax.random.key(seed), 14)
    return {
        "inputs": bell_draw(splits[0], (TOKENS, D), 1.0, 6.0, ((0, 32),)),
        "out_grad": bell_draw(splits[1], (TOKENS, D), 1.0, 6.0, ((0, 32),)),
        "offsets": draw_offsets(jax.random.fold_in(splits[13], 71), 0),
        "key_keep": place_ends((jax.random.randint(splits[3], (TOKENS,), 0, 8) < 7).astype(jnp.int32), jax.random.fold_in(splits[3], 1), 0, 1),
        "project_weight": bell_draw(splits[4], (D, 3, D), D ** -0.5, 0.21875, ((2, 4),)),
        "project_bias": bell_draw(splits[5], (2, D), 0.5, 3.0, ((1, 4),)),
        "output_weight": bell_draw(splits[6], (D, D), (D // 32) ** -0.5, 1.25, ((0, 4),)),
        "output_bias": bell_draw(splits[7], (2, D), 0.5, 3.0),
        "norm_gains": jnp.clip(1.0 + 0.18 * jax.random.normal(splits[8], (2, D), jnp.float32), 0.099609375, 1.8984375).astype(jnp.bfloat16),
        "norm_shifts": bell_draw(splits[9], (2, D), 0.5, 3.0),
        "up_weight": bell_draw(splits[10], (D, FF), D ** -0.5, 0.21875, ((1, 4),)),
        "up_bias": bell_draw(splits[11], (FF,), 0.5, 3.0, ((0, 4),)),
        "down_weight": bell_draw(splits[12], (FF, D), FF ** -0.5, 0.109375, ((0, 4),)),
    }


@jax.custom_vjp
def low(v):
    return lax.optimization_barrier(v.astype(jnp.bfloat16)).astype(jnp.float32)

@jax.custom_vjp
def low_back(v):
    return v

def low_keep(v):
    return (low(v), None)

def low_pass(kept, grad):
    return (grad,)

def back_keep(v):
    return (v, None)

def back_low(kept, grad):
    return (low(grad),)
low.defvjp(low_keep, low_pass)
low_back.defvjp(back_keep, back_low)
norm_epsilon = 1e-12
big_negative = -1e+30

def product(left, right):
    return jnp.dot(left, right, precision=lax.Precision.HIGHEST, preferred_element_type=jnp.float32)

def norm_rows(resid, gain, shift):
    center = resid - lax.optimization_barrier(jnp.mean(resid, axis=-1, keepdims=True))
    spread = lax.optimization_barrier(jnp.mean(center * center, axis=-1, keepdims=True))
    return center * lax.rsqrt(spread + norm_epsilon) * gain + shift

def gelu_exact(value):
    return jax.nn.gelu(value, approximate=False)

def slot_masks(offsets):
    position = jnp.arange(SLOT, dtype=jnp.int32)[None, :]
    segment = (position >= offsets[:, 0:1]).astype(jnp.int32) + (position >= offsets[:, 1:2]).astype(jnp.int32)
    seg_start = (position == 0) | (position == offsets[:, 0:1]) | (position == offsets[:, 1:2])
    return (segment, seg_start)

def attend_slot(pieces):
    query_slot, key_slot, value_slot, seg_row, start_row, keep_row = pieces
    raw_scores = jnp.einsum('qhd,khd->hqk', query_slot, key_slot, precision=lax.Precision.HIGHEST)
    scores = low_back(raw_scores * HD ** (-0.5))
    allowed = (seg_row[:, None] == seg_row[None, :]) & ((keep_row[None, :] == 1) | start_row[None, :])
    scores = jnp.where(allowed[None], scores, big_negative)
    probs = jax.nn.softmax(scores, axis=-1)
    return jnp.einsum('hqk,khd->qhd', low(probs), value_slot, precision=lax.Precision.HIGHEST)

def layer_group(group_in, project_weight, project_bias, output_weight, output_bias, norm_gains, norm_shifts, up_weight, up_bias, down_weight, segment, seg_start, keep_slots, live_mask):
    group_rows = group_in.shape[0]
    projected = jnp.einsum('nd,dcm->ncm', group_in, project_weight, precision=lax.Precision.HIGHEST)
    query_rows = low_back(low(projected[:, 0] + project_bias[0]))
    key_rows = low_back(low(projected[:, 1]))
    value_rows = low_back(low(projected[:, 2] + project_bias[1]))
    slot_shape = (SEQ_DP, SLOT, HEADS, HD)
    context = lax.map(jax.checkpoint(attend_slot), (query_rows.reshape(slot_shape), key_rows.reshape(slot_shape), value_rows.reshape(slot_shape), segment, seg_start, keep_slots))
    context = low_back(low(context.reshape(group_rows, D)))
    attended = low_back(product(context, output_weight))
    resid_one = group_in + attended + output_bias[0]
    normed_one = norm_rows(resid_one, norm_gains[0], norm_shifts[0])
    pre_act = low_back(product(low(normed_one), up_weight) + up_bias)
    activated = low(gelu_exact(pre_act))
    ffn_out = low_back(product(activated, down_weight))
    resid_two = normed_one + ffn_out + output_bias[1]
    return norm_rows(resid_two, norm_gains[1], norm_shifts[1]) * live_mask[:, None]

def reference(inputs, out_grad, offsets, key_keep, project_weight, project_bias, output_weight, output_bias, norm_gains, norm_shifts, up_weight, up_bias, down_weight):
    group_count = SEQS // SEQ_DP
    group_rows = SEQ_DP * SLOT
    params = tuple((p.astype(jnp.float32) for p in (project_weight, project_bias, output_weight, output_bias, norm_gains, norm_shifts, up_weight, up_bias, down_weight)))
    input_groups = inputs.astype(jnp.float32).reshape(group_count, group_rows, D)
    grad_groups = out_grad.astype(jnp.float32).reshape(group_count, group_rows, D)
    offset_groups = offsets.reshape(group_count, SEQ_DP, 2)
    keep_groups = key_keep.reshape(group_count, SEQ_DP, SLOT)

    def group_step(totals, group_item):
        group_in, group_grad, group_offsets, group_keep = group_item
        segment, seg_start = slot_masks(group_offsets)
        live_mask = (segment < 2).astype(jnp.float32).reshape(group_rows)

        def forward_group(value_in, *weights):
            return layer_group(value_in, *weights, segment, seg_start, group_keep, live_mask)
        layer_out, pullback = jax.vjp(forward_group, group_in, *params)
        gradients = pullback(group_grad)
        totals = tuple((total + grad for total, grad in zip(totals, gradients[1:])))
        return (totals, (layer_out.astype(jnp.bfloat16), gradients[0].astype(jnp.bfloat16)))
    zero_grads = tuple((jnp.zeros_like(p) for p in params))
    totals, (outputs, input_grads) = lax.scan(group_step, zero_grads, (input_groups, grad_groups, offset_groups, keep_groups))
    return (outputs.reshape(TOKENS, D), input_grads.reshape(TOKENS, D), totals[0], totals[1], totals[2], totals[3], totals[4], totals[5], totals[6], totals[7], totals[8])
```

```python
import jax
import jax.numpy as jnp
from jax import lax
from jax.sharding import PartitionSpec as P

HD = 64
SLOT = 512

norm_epsilon = 1e-12
big_negative = -1e30
low = jnp.bfloat16
wide = jnp.float32


def bits_of(size):
    return [1 << place for place in range(size.bit_length() - 1)]


def swap(value, axis, bit):
    size = lax.axis_size(axis)
    return lax.ppermute(value, axis, [(index, index ^ bit) for index in range(size)])


def upper(axis, bit):
    return (lax.axis_index(axis) & bit) != 0


def norm_parts(resid):
    center = resid - jnp.mean(resid, axis=-1, keepdims=True)
    scale = lax.rsqrt(jnp.mean(center * center, axis=-1, keepdims=True) + norm_epsilon)
    return center * scale, scale


def norm_back(unit, scale, gain, grad):
    scaled = grad * gain
    back = scale * (
        scaled
        - jnp.mean(scaled, axis=-1, keepdims=True)
        - unit * jnp.mean(scaled * unit, axis=-1, keepdims=True)
    )
    return back, jnp.sum(grad * unit, axis=0), jnp.sum(grad, axis=0)


def gelu_pair(value):
    phi_sum = 0.5 * (1.0 + lax.erf(value * 0.7071067811865476))
    density = jnp.exp(-0.5 * value * value) * 0.3989422804014327
    return value * phi_sum, phi_sum + value * density


def matmul(left, right):
    return jnp.dot(left, right, preferred_element_type=wide)


def matmul_nt(left, right):
    return lax.dot_general(left, right, (((1,), (1,)), ((), ())), preferred_element_type=wide)


def matmul_tn(left, right):
    return lax.dot_general(left, right, (((0,), (0,)), ((), ())), preferred_element_type=wide)


def heads_of(rows):
    return rows.reshape(rows.shape[0], -1, HD)


def attend(query, keys, values, allowed):
    scores = jnp.einsum(
        "qhd,khd->hqk", heads_of(query), heads_of(keys), preferred_element_type=wide
    ) * HD ** (-0.5)
    scores = jnp.where(allowed[None], scores, big_negative)
    row_max = jnp.max(scores, axis=-1, keepdims=True)
    exponent = jnp.exp(scores - row_max)
    total = jnp.sum(exponent, axis=-1, keepdims=True)
    probs = (exponent / total).astype(low)
    context = jnp.einsum("hqk,khd->qhd", probs, heads_of(values), preferred_element_type=wide)
    return context.astype(low).reshape(query.shape), row_max + jnp.log(total)


def attend_back(query, keys, values, grad, log_total, allowed):
    scores = jnp.einsum(
        "qhd,khd->hqk", heads_of(query), heads_of(keys), preferred_element_type=wide
    ) * HD ** (-0.5)
    scores = jnp.where(allowed[None], scores, big_negative)
    probs = jnp.exp(scores - log_total)
    grad_heads = heads_of(grad)
    grad_probs = jnp.einsum(
        "qhd,khd->hqk", grad_heads, heads_of(values), preferred_element_type=wide
    )
    grad_value = jnp.einsum(
        "hqk,qhd->khd", probs.astype(low), grad_heads, preferred_element_type=wide
    )
    inner = jnp.sum(probs * grad_probs, axis=-1, keepdims=True)
    grad_scores = (probs * (grad_probs - inner)).astype(low)
    grad_query = jnp.einsum(
        "hqk,khd->qhd", grad_scores, heads_of(keys), preferred_element_type=wide
    ) * HD ** (-0.5)
    grad_key = jnp.einsum(
        "hqk,qhd->khd", grad_scores, heads_of(query), preferred_element_type=wide
    ) * HD ** (-0.5)
    return [part.astype(low).reshape(query.shape) for part in (grad_query, grad_key, grad_value)]


def gather_quarters(block, share):
    near, far = bits_of(lax.axis_size("tensor"))
    if share:
        half = block.shape[0] // 2
        high = upper("dp", 1)
        start = jnp.where(high, half, 0)
        mine = swap(lax.dynamic_slice_in_dim(block, start, half), "tensor", far)
        other = swap(mine, "dp", 1)
        away = jnp.concatenate(
            [jnp.where(high, other, mine), jnp.where(high, mine, other)], axis=0
        )
    else:
        away = swap(block, "tensor", far)
    return [block, swap(block, "tensor", near), away, swap(away, "tensor", near)]


def reduce_blocks(blocks):
    near, far = bits_of(lax.axis_size("tensor"))
    rows = blocks[0].shape[0]
    far_sum = blocks[2] + swap(blocks[3].astype(low), "tensor", near).astype(wide)
    far_recv = swap(far_sum.astype(low), "tensor", far)
    total = blocks[0] + swap(blocks[1].astype(low), "tensor", near).astype(wide)
    total = total + far_recv.astype(wide)
    places = bits_of(lax.axis_size("dp"))
    for bit in places:
        half = total.shape[0] // 2
        high = upper("dp", bit)
        keep = lax.dynamic_slice_in_dim(total, jnp.where(high, half, 0), half)
        send = lax.dynamic_slice_in_dim(total, jnp.where(high, 0, half), half)
        total = keep + swap(send.astype(low), "dp", bit).astype(wide)
    total = total.astype(low)
    for bit in reversed(places):
        other = swap(total, "dp", bit)
        high = upper("dp", bit)
        total = jnp.concatenate(
            [jnp.where(high, other, total), jnp.where(high, total, other)], axis=0
        )
    assert total.shape[0] == rows
    return total.astype(wide)


def sum_everywhere(value, axis):
    for bit in bits_of(lax.axis_size(axis)):
        value = value + swap(value, axis, bit)
    return value


def shards(
    inputs,
    out_grad,
    offsets,
    key_keep,
    project_weight,
    project_bias,
    output_weight,
    output_bias,
    norm_gains,
    norm_shifts,
    up_weight,
    up_bias,
    down_weight,
):
    width = inputs.shape[1]
    local_width = project_weight.shape[2]
    units = up_weight.shape[1]
    slot = lax.axis_index("tensor")
    ends = lax.dynamic_slice_in_dim(offsets, slot, 1)
    keep_row = lax.dynamic_slice_in_dim(key_keep, slot * SLOT, SLOT)
    position = jnp.arange(SLOT, dtype=jnp.int32)
    segment = (position >= ends[0, 0]).astype(jnp.int32) + (position >= ends[0, 1]).astype(
        jnp.int32
    )
    seg_start = (position == 0) | (position == ends[0, 0]) | (position == ends[0, 1])
    allowed = (segment[:, None] == segment[None, :]) & ((keep_row == 1) | seg_start)[None, :]
    live_mask = (segment < 2).astype(wide)[:, None]
    biases = output_bias.astype(wide)
    gains = norm_gains.astype(wide)
    shifts = norm_shifts.astype(wide)

    bias_block = jnp.concatenate([project_bias.reshape(1, -1), up_bias.reshape(1, -1)], axis=1)
    bias_parts = gather_quarters(bias_block, False)
    attn_block = jnp.concatenate(
        [project_weight.reshape(width, 3 * local_width).T, output_weight], axis=0
    )
    attn_parts = gather_quarters(attn_block, True)
    up_parts = gather_quarters(up_weight, True)
    down_parts = gather_quarters(down_weight, True)
    count = len(attn_parts)

    saved = []
    attended = 0.0
    for part in range(count):
        bias = bias_parts[part][0].astype(wide)
        rows = matmul_nt(inputs, attn_parts[part][: 3 * local_width])
        query = (rows[:, :local_width] + bias[:local_width]).astype(low)
        keys = rows[:, local_width : 2 * local_width].astype(low)
        values = (rows[:, 2 * local_width :] + bias[local_width : 2 * local_width]).astype(low)
        context, log_total = attend(query, keys, values, allowed)
        attended = attended + matmul(context, attn_parts[part][3 * local_width :])
        saved.append((query, keys, values, context, log_total))

    resid_one = inputs.astype(wide) + attended + biases[0]
    unit_one, scale_one = norm_parts(resid_one)
    normed_one = unit_one * gains[0] + shifts[0]
    normed_low = normed_one.astype(low)
    ffn_out = 0.0
    kept = []
    for part in range(count):
        bias = bias_parts[part][0, 2 * local_width :].astype(wide)
        active, slope = gelu_pair(matmul(normed_low, up_parts[part]) + bias)
        active = active.astype(low)
        ffn_out = ffn_out + matmul(active, down_parts[part])
        kept.append((active, slope))
    resid_two = normed_one + ffn_out + biases[1]
    unit_two, scale_two = norm_parts(resid_two)
    layer_output = ((unit_two * gains[1] + shifts[1]) * live_mask).astype(low)

    grad_out = out_grad.astype(wide) * live_mask
    grad_two, gain_two, shift_two = norm_back(unit_two, scale_two, gains[1], grad_out)
    grad_ffn = grad_two.astype(low)
    grad_one_in = grad_two
    grad_pres = []
    for part in range(count):
        grad_act = matmul_nt(grad_ffn, down_parts[part])
        grad_pre = (grad_act * kept[part][1]).astype(low)
        grad_pres.append(grad_pre)
        grad_one_in = grad_one_in + matmul_nt(grad_pre, up_parts[part])
    order = [3, 2, 1, 0]
    down_grads = [matmul_tn(kept[part][0], grad_ffn) for part in range(count)]
    down_weight_grad = reduce_blocks(down_grads)
    up_grads = [matmul_tn(normed_low, grad_pres[part]) for part in range(count)]
    up_weight_grad = reduce_blocks(up_grads)
    up_bias_grads = [jnp.sum(grad_pres[part], axis=0, dtype=wide) for part in range(count)]

    grad_one, gain_one, shift_one = norm_back(unit_one, scale_one, gains[0], grad_one_in)
    grad_attended = grad_one.astype(low)
    grad_input = 0.0
    attn_grads = []
    project_bias_grads = []
    for part in range(count):
        query, keys, values, context, log_total = saved[part]
        grad_context = matmul_nt(grad_attended, attn_parts[part][3 * local_width :]).astype(low)
        pieces = attend_back(query, keys, values, grad_context, log_total, allowed)
        grad_rows = jnp.concatenate(pieces, axis=1)
        grad_input = grad_input + matmul(grad_rows, attn_parts[part][: 3 * local_width])
        attn_grads.append(
            jnp.concatenate(
                [matmul_tn(grad_rows, inputs), matmul_tn(context, grad_attended)], axis=0
            )
        )
        project_bias_grads.append(
            jnp.concatenate(
                [
                    jnp.sum(pieces[0], axis=0, dtype=wide),
                    jnp.sum(pieces[2], axis=0, dtype=wide),
                ]
            )
        )
    input_grad = (grad_one + grad_input).astype(low)
    attn_grad = reduce_blocks(attn_grads)
    project_weight_grad = attn_grad[: 3 * local_width].T.reshape(width, 3, local_width)
    output_weight_grad = attn_grad[3 * local_width :]

    near, far = bits_of(lax.axis_size("tensor"))
    small = [
        jnp.concatenate([project_bias_grads[part], up_bias_grads[part]]) for part in range(count)
    ]
    pair = jnp.concatenate([small[0], small[2]]) + swap(
        jnp.concatenate([small[1], small[3]]), "tensor", near
    )
    length = small[0].shape[0]
    own_small = pair[:length] + swap(pair[length:], "tensor", far)
    shared = jnp.concatenate(
        [jnp.sum(grad_one, axis=0), jnp.sum(grad_two, axis=0), gain_one, gain_two, shift_one, shift_two]
    )
    shared = sum_everywhere(shared, "tensor")
    packed = sum_everywhere(jnp.concatenate([own_small, shared]), "dp")
    project_bias_grad = packed[: 2 * local_width].reshape(2, local_width)
    up_bias_grad = packed[2 * local_width : length]
    norm_grads = packed[length:].reshape(3, 2, width)
    return (
        layer_output,
        input_grad,
        project_weight_grad,
        project_bias_grad,
        output_weight_grad,
        norm_grads[0],
        norm_grads[1],
        norm_grads[2],
        up_weight_grad,
        up_bias_grad,
        down_weight_grad,
    )


def solution(mesh):
    in_specs = (
        P(("dp", "tensor"), None),
        P(("dp", "tensor"), None),
        P("dp", None),
        P("dp"),
        P(None, None, "tensor"),
        P(None, "tensor"),
        P("tensor", None),
        P(),
        P(),
        P(),
        P(None, "tensor"),
        P("tensor"),
        P("tensor", None),
    )
    out_specs = (
        P(("dp", "tensor"), None),
        P(("dp", "tensor"), None),
        P(None, None, "tensor"),
        P(None, "tensor"),
        P("tensor", None),
        P(),
        P(),
        P(),
        P(None, "tensor"),
        P("tensor"),
        P("tensor", None),
    )
    return jax.shard_map(shards, mesh=mesh, in_specs=in_specs, out_specs=out_specs, check_vma=False)
```

```python
import jax
import jax.numpy as jnp
from jax import lax
from jax.sharding import PartitionSpec as P

HD = 64
SLOT = 512

norm_epsilon = 1e-12
big_negative = -1e30
low = jnp.bfloat16
wide = jnp.float32


def bits_of(size):
    return [1 << place for place in range(size.bit_length() - 1)]


def swap(value, axis, bit):
    size = lax.axis_size(axis)
    return lax.ppermute(value, axis, [(index, index ^ bit) for index in range(size)])


def upper(axis, bit):
    return (lax.axis_index(axis) & bit) != 0


def norm_parts(resid):
    center = resid - jnp.mean(resid, axis=-1, keepdims=True)
    scale = lax.rsqrt(jnp.mean(center * center, axis=-1, keepdims=True) + norm_epsilon)
    return center * scale, scale


def norm_back(unit, scale, gain, grad):
    scaled = grad * gain
    back = scale * (
        scaled
        - jnp.mean(scaled, axis=-1, keepdims=True)
        - unit * jnp.mean(scaled * unit, axis=-1, keepdims=True)
    )
    return back, jnp.sum(grad * unit, axis=0), jnp.sum(grad, axis=0)


def gelu_pair(value):
    phi_sum = 0.5 * (1.0 + lax.erf(value * 0.7071067811865476))
    density = jnp.exp(-0.5 * value * value) * 0.3989422804014327
    return value * phi_sum, phi_sum + value * density


def matmul(left, right):
    return jnp.dot(left, right, preferred_element_type=wide)


def matmul_nt(left, right):
    return lax.dot_general(left, right, (((1,), (1,)), ((), ())), preferred_element_type=wide)


def matmul_tn(left, right):
    return lax.dot_general(left, right, (((0,), (0,)), ((), ())), preferred_element_type=wide)


def heads_of(rows):
    return rows.reshape(rows.shape[0], -1, HD)


def attend(query, keys, values, allowed):
    scores = jnp.einsum(
        "qhd,khd->hqk", heads_of(query), heads_of(keys), preferred_element_type=wide
    ) * HD ** (-0.5)
    scores = jnp.where(allowed[None], scores, big_negative)
    row_max = jnp.max(scores, axis=-1, keepdims=True)
    exponent = jnp.exp(scores - row_max)
    total = jnp.sum(exponent, axis=-1, keepdims=True)
    probs = (exponent / total).astype(low)
    context = jnp.einsum("hqk,khd->qhd", probs, heads_of(values), preferred_element_type=wide)
    return context.astype(low).reshape(query.shape), row_max + jnp.log(total)


def attend_back(query, keys, values, grad, log_total, allowed):
    scores = jnp.einsum(
        "qhd,khd->hqk", heads_of(query), heads_of(keys), preferred_element_type=wide
    ) * HD ** (-0.5)
    scores = jnp.where(allowed[None], scores, big_negative)
    probs = jnp.exp(scores - log_total)
    grad_heads = heads_of(grad)
    grad_probs = jnp.einsum(
        "qhd,khd->hqk", grad_heads, heads_of(values), preferred_element_type=wide
    )
    grad_value = jnp.einsum(
        "hqk,qhd->khd", probs.astype(low), grad_heads, preferred_element_type=wide
    )
    inner = jnp.sum(probs * grad_probs, axis=-1, keepdims=True)
    grad_scores = (probs * (grad_probs - inner)).astype(low)
    grad_query = jnp.einsum(
        "hqk,khd->qhd", grad_scores, heads_of(keys), preferred_element_type=wide
    ) * HD ** (-0.5)
    grad_key = jnp.einsum(
        "hqk,qhd->khd", grad_scores, heads_of(query), preferred_element_type=wide
    ) * HD ** (-0.5)
    return [part.astype(low).reshape(query.shape) for part in (grad_query, grad_key, grad_value)]


def gate(*values):
    return lax.optimization_barrier(values)


def fetch_far(block, after):
    far = bits_of(lax.axis_size("tensor"))[1]
    half = block.shape[0] // 2
    high = upper("dp", 1)
    piece = lax.dynamic_slice_in_dim(block, jnp.where(high, half, 0), half)
    if after is not None:
        piece, after = gate(piece, after)
    return swap(piece, "tensor", far), after


def spread(mine, block):
    near = bits_of(lax.axis_size("tensor"))[0]
    high = upper("dp", 1)
    other = swap(mine, "dp", 1)
    away = jnp.concatenate([jnp.where(high, other, mine), jnp.where(high, mine, other)], axis=0)
    return [block, swap(block, "tensor", near), away, swap(away, "tensor", near)]


def near_sum(keep, send):
    near = bits_of(lax.axis_size("tensor"))[0]
    return keep + swap(send, "tensor", near).astype(wide)


def far_sum(keep, send):
    far = bits_of(lax.axis_size("tensor"))[1]
    return keep + swap(send, "tensor", far).astype(wide)


def halve(total, bit):
    half = total.shape[0] // 2
    high = upper("dp", bit)
    keep = lax.dynamic_slice_in_dim(total, jnp.where(high, half, 0), half)
    send = lax.dynamic_slice_in_dim(total, jnp.where(high, 0, half), half)
    return keep + swap(send.astype(low), "dp", bit).astype(wide)


def finish(total, start):
    places = bits_of(lax.axis_size("dp"))
    for bit in places[start:]:
        total = halve(total, bit)
    total = total.astype(low)
    for bit in reversed(places):
        other = swap(total, "dp", bit)
        high = upper("dp", bit)
        total = jnp.concatenate(
            [jnp.where(high, other, total), jnp.where(high, total, other)], axis=0
        )
    return total.astype(wide)


def sum_everywhere(value, axis):
    for bit in bits_of(lax.axis_size(axis)):
        value = value + swap(value, axis, bit)
    return value


def shards(
    inputs,
    out_grad,
    offsets,
    key_keep,
    project_weight,
    project_bias,
    output_weight,
    output_bias,
    norm_gains,
    norm_shifts,
    up_weight,
    up_bias,
    down_weight,
):
    width = inputs.shape[1]
    local_width = project_weight.shape[2]
    units = up_weight.shape[1]
    slot = lax.axis_index("tensor")
    ends = lax.dynamic_slice_in_dim(offsets, slot, 1)
    keep_row = lax.dynamic_slice_in_dim(key_keep, slot * SLOT, SLOT)
    position = jnp.arange(SLOT, dtype=jnp.int32)
    segment = (position >= ends[0, 0]).astype(jnp.int32) + (position >= ends[0, 1]).astype(
        jnp.int32
    )
    seg_start = (position == 0) | (position == ends[0, 0]) | (position == ends[0, 1])
    allowed = (segment[:, None] == segment[None, :]) & ((keep_row == 1) | seg_start)[None, :]
    live_mask = (segment < 2).astype(wide)[:, None]
    biases = output_bias.astype(wide)
    gains = norm_gains.astype(wide)
    shifts = norm_shifts.astype(wide)

    own_bias = jnp.concatenate([project_bias.reshape(-1), up_bias])
    lines = -(-own_bias.shape[0] // width)
    bias_rows = jnp.pad(own_bias, (0, 16 * width - own_bias.shape[0])).reshape(16, width)
    attn_block = jnp.concatenate(
        [project_weight.reshape(width, 3 * local_width).T, output_weight, bias_rows], axis=0
    )
    attn_far, _ = fetch_far(attn_block, None)
    up_far, attn_far = fetch_far(up_weight, attn_far)
    attn_parts = spread(attn_far, attn_block)
    down_far, up_far = fetch_far(down_weight, up_far)
    up_parts = spread(up_far, up_weight)
    down_parts = spread(down_far, down_weight)
    count = len(attn_parts)
    edge = 3 * local_width + output_weight.shape[0]
    bias_parts = [part[edge : edge + lines].reshape(1, -1) for part in attn_parts]

    saved = []
    attended = 0.0
    for part in range(count):
        bias = bias_parts[part][0].astype(wide)
        rows = matmul_nt(inputs, attn_parts[part][: 3 * local_width])
        query = (rows[:, :local_width] + bias[:local_width]).astype(low)
        keys = rows[:, local_width : 2 * local_width].astype(low)
        values = (rows[:, 2 * local_width :] + bias[local_width : 2 * local_width]).astype(low)
        context, log_total = attend(query, keys, values, allowed)
        attended = attended + matmul(context, attn_parts[part][3 * local_width : edge])
        saved.append((query, keys, values, context, log_total))

    resid_one = inputs.astype(wide) + attended + biases[0]
    unit_one, scale_one = norm_parts(resid_one)
    normed_one = unit_one * gains[0] + shifts[0]
    normed_low = normed_one.astype(low)
    ffn_out = 0.0
    kept = []
    for part in range(count):
        bias = bias_parts[part][0, 2 * local_width : 2 * local_width + units].astype(wide)
        active, slope = gelu_pair(matmul(normed_low, up_parts[part]) + bias)
        active = active.astype(low)
        ffn_out = ffn_out + matmul(active, down_parts[part])
        kept.append((active, slope))
    resid_two = normed_one + ffn_out + biases[1]
    unit_two, scale_two = norm_parts(resid_two)
    layer_output = ((unit_two * gains[1] + shifts[1]) * live_mask).astype(low)

    grad_out = out_grad.astype(wide) * live_mask
    grad_two, gain_two, shift_two = norm_back(unit_two, scale_two, gains[1], grad_out)
    grad_ffn = grad_two.astype(low)
    down_grads = [matmul_tn(kept[part][0], grad_ffn) for part in range(count)]
    down_three, down_one, grad_ffn = gate(
        down_grads[3].astype(low), down_grads[1].astype(low), grad_ffn
    )
    down_far_sum = near_sum(down_grads[2], down_three)
    down_total = near_sum(down_grads[0], down_one)
    grad_one_in = grad_two
    grad_pres = []
    for part in range(count):
        grad_act = matmul_nt(grad_ffn, down_parts[part])
        grad_pre = (grad_act * kept[part][1]).astype(low)
        grad_pres.append(grad_pre)
        grad_one_in = grad_one_in + matmul_nt(grad_pre, up_parts[part])
    down_far_low, grad_one_in, down_total = gate(
        down_far_sum.astype(low), grad_one_in, down_total
    )
    down_total = far_sum(down_total, down_far_low)
    up_grads = [matmul_tn(normed_low, grad_pres[part]) for part in range(count)]
    up_three, up_one, grad_one_in = gate(
        up_grads[3].astype(low), up_grads[1].astype(low), grad_one_in
    )
    up_far_sum = near_sum(up_grads[2], up_three)
    up_total = near_sum(up_grads[0], up_one)
    up_bias_grads = [jnp.sum(grad_pres[part], axis=0, dtype=wide) for part in range(count)]

    grad_one, gain_one, shift_one = norm_back(unit_one, scale_one, gains[0], grad_one_in)
    grad_attended = grad_one.astype(low)
    grad_input = 0.0
    attn_grads = {}
    project_bias_grads = {}
    for part in (3, 2, 1, 0):
        query, keys, values, context, log_total = saved[part]
        grad_context = matmul_nt(
            grad_attended, attn_parts[part][3 * local_width : edge]
        ).astype(low)
        pieces = attend_back(query, keys, values, grad_context, log_total, allowed)
        grad_rows = jnp.concatenate(pieces, axis=1)
        grad_input = grad_input + matmul(grad_rows, attn_parts[part][: 3 * local_width])
        attn_grads[part] = jnp.concatenate(
            [matmul_tn(grad_rows, inputs), matmul_tn(context, grad_attended)], axis=0
        )
        project_bias_grads[part] = jnp.concatenate(
            [jnp.sum(pieces[0], axis=0, dtype=wide), jnp.sum(pieces[2], axis=0, dtype=wide)]
        )
        if part == 3:
            attn_three, up_far_low, up_total, down_total, grad_attended = gate(
                attn_grads[3].astype(low),
                up_far_sum.astype(low),
                up_total,
                down_total,
                grad_attended,
            )
            up_total = far_sum(up_total, up_far_low)
            down_total = halve(down_total, 1)
        elif part == 2:
            attn_far_sum = near_sum(attn_grads[2], attn_three)
            attn_far_low, down_total, grad_attended = gate(
                attn_far_sum.astype(low), down_total, grad_attended
            )
        elif part == 1:
            attn_one, up_total, grad_attended = gate(
                attn_grads[1].astype(low), up_total, grad_attended
            )
            up_total = halve(up_total, 1)
    input_grad = (grad_one + grad_input).astype(low)
    attn_total = far_sum(near_sum(attn_grads[0], attn_one), attn_far_low)
    down_weight_grad = finish(down_total, 1)
    up_weight_grad = finish(up_total, 1)
    attn_grad = finish(attn_total, 0)
    project_weight_grad = attn_grad[: 3 * local_width].T.reshape(width, 3, local_width)
    output_weight_grad = attn_grad[3 * local_width :]

    near, far = bits_of(lax.axis_size("tensor"))
    small = [
        jnp.concatenate([project_bias_grads[part], up_bias_grads[part]]) for part in range(count)
    ]
    shared = jnp.concatenate(
        [
            jnp.sum(grad_one, axis=0),
            jnp.sum(grad_two, axis=0),
            gain_one,
            gain_two,
            shift_one,
            shift_two,
        ]
    )
    length = small[0].shape[0]
    from_near = swap(jnp.concatenate([small[1], small[3], shared]), "tensor", near)
    pair = jnp.concatenate([small[0], small[2], shared]) + from_near
    from_far = swap(pair[length:], "tensor", far)
    packed = jnp.concatenate(
        [pair[:length] + from_far[:length], pair[2 * length :] + from_far[length:]]
    )
    packed = sum_everywhere(packed, "dp")
    project_bias_grad = packed[: 2 * local_width].reshape(2, local_width)
    up_bias_grad = packed[2 * local_width : length]
    norm_grads = packed[length:].reshape(3, 2, width)
    return (
        layer_output,
        input_grad,
        project_weight_grad,
        project_bias_grad,
        output_weight_grad,
        norm_grads[0],
        norm_grads[1],
        norm_grads[2],
        up_weight_grad,
        up_bias_grad,
        down_weight_grad,
    )


def solution(mesh):
    in_specs = (
        P(("dp", "tensor"), None),
        P(("dp", "tensor"), None),
        P("dp", None),
        P("dp"),
        P(None, None, "tensor"),
        P(None, "tensor"),
        P("tensor", None),
        P(),
        P(),
        P(),
        P(None, "tensor"),
        P("tensor"),
        P("tensor", None),
    )
    out_specs = (
        P(("dp", "tensor"), None),
        P(("dp", "tensor"), None),
        P(None, None, "tensor"),
        P(None, "tensor"),
        P("tensor", None),
        P(),
        P(),
        P(),
        P(None, "tensor"),
        P("tensor"),
        P("tensor", None),
    )
    return jax.shard_map(shards, mesh=mesh, in_specs=in_specs, out_specs=out_specs, check_vma=False)
```

```python
import jax
import jax.numpy as jnp
from jax import lax
from jax.sharding import PartitionSpec as P

HD = 64
SLOT = 512

norm_epsilon = 1e-12
big_negative = -1e30
low = jnp.bfloat16
wide = jnp.float32


def bits_of(size):
    return [1 << place for place in range(size.bit_length() - 1)]


def swap(value, axis, bit):
    size = lax.axis_size(axis)
    return lax.ppermute(value, axis, [(index, index ^ bit) for index in range(size)])


def upper(axis, bit):
    return (lax.axis_index(axis) & bit) != 0


def norm_parts(resid):
    center = resid - jnp.mean(resid, axis=-1, keepdims=True)
    scale = lax.rsqrt(jnp.mean(center * center, axis=-1, keepdims=True) + norm_epsilon)
    return center * scale, scale


def norm_back(unit, scale, gain, grad):
    scaled = grad * gain
    back = scale * (
        scaled
        - jnp.mean(scaled, axis=-1, keepdims=True)
        - unit * jnp.mean(scaled * unit, axis=-1, keepdims=True)
    )
    return back, jnp.sum(grad * unit, axis=0), jnp.sum(grad, axis=0)


def gelu_pair(value):
    phi_sum = 0.5 * (1.0 + lax.erf(value * 0.7071067811865476))
    density = jnp.exp(-0.5 * value * value) * 0.3989422804014327
    return value * phi_sum, phi_sum + value * density


def matmul(left, right):
    return jnp.dot(left, right, preferred_element_type=wide)


def matmul_nt(left, right):
    return lax.dot_general(left, right, (((1,), (1,)), ((), ())), preferred_element_type=wide)


def matmul_tn(left, right):
    return lax.dot_general(left, right, (((0,), (0,)), ((), ())), preferred_element_type=wide)


def heads_of(rows):
    return rows.reshape(rows.shape[0], -1, HD)


def attend(query, keys, values, allowed):
    scores = jnp.einsum(
        "qhd,khd->hqk", heads_of(query), heads_of(keys), preferred_element_type=wide
    ) * HD ** (-0.5)
    scores = jnp.where(allowed[None], scores, big_negative)
    row_max = jnp.max(scores, axis=-1, keepdims=True)
    exponent = jnp.exp(scores - row_max)
    total = jnp.sum(exponent, axis=-1, keepdims=True)
    probs = (exponent / total).astype(low)
    context = jnp.einsum("hqk,khd->qhd", probs, heads_of(values), preferred_element_type=wide)
    return context.astype(low).reshape(query.shape), row_max + jnp.log(total)


def attend_back(query, keys, values, grad, log_total, allowed):
    scores = jnp.einsum(
        "qhd,khd->hqk", heads_of(query), heads_of(keys), preferred_element_type=wide
    ) * HD ** (-0.5)
    scores = jnp.where(allowed[None], scores, big_negative)
    probs = jnp.exp(scores - log_total)
    grad_heads = heads_of(grad)
    grad_probs = jnp.einsum(
        "qhd,khd->hqk", grad_heads, heads_of(values), preferred_element_type=wide
    )
    grad_value = jnp.einsum(
        "hqk,qhd->khd", probs.astype(low), grad_heads, preferred_element_type=wide
    )
    inner = jnp.sum(probs * grad_probs, axis=-1, keepdims=True)
    grad_scores = (probs * (grad_probs - inner)).astype(low)
    grad_query = jnp.einsum(
        "hqk,khd->qhd", grad_scores, heads_of(keys), preferred_element_type=wide
    ) * HD ** (-0.5)
    grad_key = jnp.einsum(
        "hqk,qhd->khd", grad_scores, heads_of(query), preferred_element_type=wide
    ) * HD ** (-0.5)
    return [part.astype(low).reshape(query.shape) for part in (grad_query, grad_key, grad_value)]


def gate(*values):
    return lax.optimization_barrier(values)


def fetch_far(block, after):
    far = bits_of(lax.axis_size("tensor"))[1]
    half = block.shape[0] // 2
    piece = lax.dynamic_slice_in_dim(block, jnp.where(upper("dp", 1), half, 0), half)
    piece, *after = gate(piece, *after)
    return swap(piece, "tensor", far), after


def spread(mine, other):
    high = upper("dp", 1)
    away = jnp.concatenate([jnp.where(high, other, mine), jnp.where(high, mine, other)], axis=0)
    return away, swap(away, "tensor", bits_of(lax.axis_size("tensor"))[0])


def near_sum(keep, send):
    near = bits_of(lax.axis_size("tensor"))[0]
    return keep + swap(send, "tensor", near).astype(wide)


def far_sum(keep, send):
    far = bits_of(lax.axis_size("tensor"))[1]
    return keep + swap(send, "tensor", far).astype(wide)


def halve(total, bit):
    half = total.shape[0] // 2
    high = upper("dp", bit)
    keep = lax.dynamic_slice_in_dim(total, jnp.where(high, half, 0), half)
    send = lax.dynamic_slice_in_dim(total, jnp.where(high, 0, half), half)
    return keep + swap(send.astype(low), "dp", bit).astype(wide)


def grow(total, bit):
    other = swap(total, "dp", bit)
    high = upper("dp", bit)
    return jnp.concatenate(
        [jnp.where(high, other, total), jnp.where(high, total, other)], axis=0
    )


class Chain:
    def __init__(self, value, turn, far=None):
        places = bits_of(lax.axis_size("dp"))
        places = places[turn:] + places[:turn]
        self.value = value
        self.far = far
        self.stages = [lambda total, bit=bit: halve(total, bit) for bit in places]
        self.stages.append(lambda total: grow(total.astype(low), places[-1]))
        self.stages += [lambda total, bit=bit: grow(total, bit) for bit in places[-2::-1]]

    def step(self):
        if self.far is not None:
            self.value = far_sum(self.value, self.far)
            self.far = None
        elif self.stages:
            self.value = self.stages.pop(0)(self.value)

    def finish(self):
        while self.far is not None or self.stages:
            self.step()
        return self.value.astype(wide)


class Spread:
    def __init__(self, value):
        self.value = value
        self.far = None
        self.stages = [
            (axis, bit) for axis in ("tensor", "dp") for bit in bits_of(lax.axis_size(axis))
        ]

    def step(self):
        if self.stages:
            self.value = self.value + swap(self.value, *self.stages.pop(0))

    def finish(self):
        while self.stages:
            self.step()
        return self.value


def hold(extra, chains):
    held = [value for chain in chains for value in (chain.value, chain.far) if value is not None]
    extra_out = gate(*extra, *held)
    held = list(extra_out[len(extra) :])
    for chain in chains:
        chain.value = held.pop(0)
        if chain.far is not None:
            chain.far = held.pop(0)
    return extra_out[: len(extra)]


def in_turn(parts):
    size = lax.axis_size("tensor")
    slot = lax.axis_index("tensor")
    stacked = jnp.stack([parts[part] for part in range(size)])
    for bit in bits_of(size):
        flipped = jnp.stack([stacked[part ^ bit] for part in range(size)])
        stacked = jnp.where((slot & bit) != 0, flipped, stacked)
    return [stacked.reshape(-1)]


def shards(
    inputs,
    out_grad,
    offsets,
    key_keep,
    project_weight,
    project_bias,
    output_weight,
    output_bias,
    norm_gains,
    norm_shifts,
    up_weight,
    up_bias,
    down_weight,
):
    width = inputs.shape[1]
    local_width = project_weight.shape[2]
    units = up_weight.shape[1]
    slot = lax.axis_index("tensor")
    ends = lax.dynamic_slice_in_dim(offsets, slot, 1)
    keep_row = lax.dynamic_slice_in_dim(key_keep, slot * SLOT, SLOT)
    position = jnp.arange(SLOT, dtype=jnp.int32)
    segment = (position >= ends[0, 0]).astype(jnp.int32) + (position >= ends[0, 1]).astype(
        jnp.int32
    )
    seg_start = (position == 0) | (position == ends[0, 0]) | (position == ends[0, 1])
    allowed = (segment[:, None] == segment[None, :]) & ((keep_row == 1) | seg_start)[None, :]
    live_mask = (segment < 2).astype(wide)[:, None]
    biases = output_bias.astype(wide)
    gains = norm_gains.astype(wide)
    shifts = norm_shifts.astype(wide)

    own_bias = jnp.concatenate([project_bias.reshape(-1), up_bias])
    lines = -(-own_bias.shape[0] // width)
    bias_rows = jnp.pad(own_bias, (0, 16 * width - own_bias.shape[0])).reshape(16, width)
    attn_block = jnp.concatenate(
        [project_weight.reshape(width, 3 * local_width).T, output_weight, bias_rows], axis=0
    )
    near = bits_of(lax.axis_size("tensor"))[0]
    attn_near = swap(attn_block, "tensor", near)
    attn_far, _ = fetch_far(attn_block, ())
    up_far, (attn_far,) = fetch_far(up_weight, (attn_far,))
    attn_other = swap(attn_far, "dp", 1)
    up_near = swap(up_weight, "tensor", near)
    down_near = swap(down_weight, "tensor", near)
    attn_parts = [attn_block, attn_near]
    edge = 3 * local_width + output_weight.shape[0]
    count = 4

    def bias_of(part):
        return attn_parts[part][edge : edge + lines].reshape(1, -1)

    saved = []
    attended = 0.0
    for part in range(count):
        if part == 2:
            down_far, (up_far, attended, attn_other) = fetch_far(
                down_weight, (up_far, attended, attn_other)
            )
            attn_parts += spread(attn_far, attn_other)
            up_other = swap(up_far, "dp", 1)
        if part == 3:
            down_far, up_other, attended = gate(down_far, up_other, attended)
            down_other = swap(down_far, "dp", 1)
        bias = bias_of(part)[0].astype(wide)
        rows = matmul_nt(inputs, attn_parts[part][: 3 * local_width])
        query = (rows[:, :local_width] + bias[:local_width]).astype(low)
        keys = rows[:, local_width : 2 * local_width].astype(low)
        values = (rows[:, 2 * local_width :] + bias[local_width : 2 * local_width]).astype(low)
        context, log_total = attend(query, keys, values, allowed)
        attended = attended + matmul(context, attn_parts[part][3 * local_width : edge])
        saved.append((query, keys, values, context, log_total))

    up_other, attended = gate(up_other, attended)
    up_parts = [up_weight, up_near, *spread(up_far, up_other)]
    down_parts = [down_weight, down_near]
    resid_one = inputs.astype(wide) + attended + biases[0]
    unit_one, scale_one = norm_parts(resid_one)
    normed_one = unit_one * gains[0] + shifts[0]
    normed_low = normed_one.astype(low)
    ffn_out = 0.0
    kept = []
    for part in range(count):
        if part == 1:
            down_other, ffn_out = gate(down_other, ffn_out)
            down_parts += spread(down_far, down_other)
        bias = bias_of(part)[0, 2 * local_width : 2 * local_width + units].astype(wide)
        active, slope = gelu_pair(matmul(normed_low, up_parts[part]) + bias)
        active = active.astype(low)
        ffn_out = ffn_out + matmul(active, down_parts[part])
        kept.append((active, slope))
    resid_two = normed_one + ffn_out + biases[1]
    unit_two, scale_two = norm_parts(resid_two)
    layer_output = ((unit_two * gains[1] + shifts[1]) * live_mask).astype(low)

    grad_out = out_grad.astype(wide) * live_mask
    grad_two, gain_two, shift_two = norm_back(unit_two, scale_two, gains[1], grad_out)
    grad_ffn = grad_two.astype(low)
    down_grads = [matmul_tn(kept[part][0], grad_ffn) for part in range(count)]
    down_three, down_one, grad_ffn = gate(
        down_grads[3].astype(low), down_grads[1].astype(low), grad_ffn
    )
    down_far_sum = near_sum(down_grads[2], down_three)
    down_total = near_sum(down_grads[0], down_one)
    grad_one_in = grad_two
    grad_pres = []
    for part in range(count):
        grad_act = matmul_nt(grad_ffn, down_parts[part])
        grad_pre = (grad_act * kept[part][1]).astype(low)
        grad_pres.append(grad_pre)
        grad_one_in = grad_one_in + matmul_nt(grad_pre, up_parts[part])
    down_chain = Chain(down_total, 0, down_far_sum.astype(low))
    (grad_one_in,) = hold((grad_one_in,), [down_chain])
    down_chain.step()
    up_grads = [matmul_tn(normed_low, grad_pres[part]) for part in range(count)]
    up_three, up_one, grad_one_in = gate(
        up_grads[3].astype(low), up_grads[1].astype(low), grad_one_in
    )
    up_far_sum = near_sum(up_grads[2], up_three)
    up_chain = Chain(near_sum(up_grads[0], up_one), 1, up_far_sum.astype(low))
    up_bias_grads = [jnp.sum(grad_pres[part], axis=0, dtype=wide) for part in range(count)]

    grad_one, gain_one, shift_one = norm_back(unit_one, scale_one, gains[0], grad_one_in)
    grad_attended = grad_one.astype(low)
    early = [jnp.sum(grad_one, axis=0), jnp.sum(grad_two, axis=0)]
    early += [gain_one, gain_two, shift_one, shift_two]
    early_chain = Spread(jnp.concatenate(early + in_turn(up_bias_grads)))
    grad_input = 0.0
    attn_grads = {}
    project_bias_grads = {}
    for part in (3, 2, 1, 0):
        query, keys, values, context, log_total = saved[part]
        grad_context = matmul_nt(
            grad_attended, attn_parts[part][3 * local_width : edge]
        ).astype(low)
        pieces = attend_back(query, keys, values, grad_context, log_total, allowed)
        grad_rows = jnp.concatenate(pieces, axis=1)
        grad_input = grad_input + matmul(grad_rows, attn_parts[part][: 3 * local_width])
        attn_grads[part] = jnp.concatenate(
            [matmul_tn(grad_rows, inputs), matmul_tn(context, grad_attended)], axis=0
        )
        project_bias_grads[part] = jnp.concatenate(
            [jnp.sum(pieces[0], axis=0, dtype=wide), jnp.sum(pieces[2], axis=0, dtype=wide)]
        )
        if part == 3:
            attn_three, grad_attended = hold(
                (attn_grads[3].astype(low), grad_attended), [up_chain, down_chain, early_chain]
            )
            up_chain.step()
            down_chain.step()
            early_chain.step()
            attn_far_sum = None
        elif part == 2:
            attn_far_sum = near_sum(attn_grads[2], attn_three).astype(low)
            attn_far_sum, grad_attended = hold(
                (attn_far_sum, grad_attended), [down_chain, early_chain]
            )
            attn_recv = swap(attn_far_sum, "tensor", bits_of(lax.axis_size("tensor"))[1])
            down_chain.step()
            early_chain.step()
        elif part == 1:
            attn_one, grad_attended = hold(
                (attn_grads[1].astype(low), grad_attended), [up_chain, down_chain, early_chain]
            )
            attn_total = near_sum(0.0, attn_one)
            up_chain.step()
            down_chain.step()
            early_chain.step()
    late_chain = Spread(jnp.concatenate(in_turn(project_bias_grads)))
    attn_total = attn_grads[0] + attn_total
    grad_input, attn_recv, attn_total = hold(
        (grad_input, attn_recv, attn_total), [up_chain, down_chain, early_chain, late_chain]
    )
    attn_total = attn_total + attn_recv.astype(wide)
    half = attn_total.shape[0] // 2
    attn_chains = [Chain(attn_total[:half], 0), Chain(attn_total[half:], 1)]
    input_grad = (grad_one + grad_input).astype(low)
    busy = attn_chains + [up_chain, down_chain, early_chain, late_chain]
    while any(chain.stages for chain in busy):
        for chain in busy:
            chain.step()
    down_weight_grad = down_chain.finish()
    up_weight_grad = up_chain.finish()
    attn_grad = jnp.concatenate([chain.finish() for chain in attn_chains], axis=0)
    project_weight_grad = attn_grad[: 3 * local_width].T.reshape(width, 3, local_width)
    output_weight_grad = attn_grad[3 * local_width :]
    early_sum = early_chain.finish()
    norm_grads = early_sum[: 6 * width].reshape(3, 2, width)
    up_bias_grad = lax.dynamic_slice_in_dim(early_sum, 6 * width + slot * units, units)
    late_sum = late_chain.finish()
    project_bias_grad = lax.dynamic_slice_in_dim(
        late_sum, slot * 2 * local_width, 2 * local_width
    ).reshape(2, local_width)
    return (
        layer_output,
        input_grad,
        project_weight_grad,
        project_bias_grad,
        output_weight_grad,
        norm_grads[0],
        norm_grads[1],
        norm_grads[2],
        up_weight_grad,
        up_bias_grad,
        down_weight_grad,
    )


def solution(mesh):
    in_specs = (
        P(("dp", "tensor"), None),
        P(("dp", "tensor"), None),
        P("dp", None),
        P("dp"),
        P(None, None, "tensor"),
        P(None, "tensor"),
        P("tensor", None),
        P(),
        P(),
        P(),
        P(None, "tensor"),
        P("tensor"),
        P("tensor", None),
    )
    out_specs = (
        P(("dp", "tensor"), None),
        P(("dp", "tensor"), None),
        P(None, None, "tensor"),
        P(None, "tensor"),
        P("tensor", None),
        P(),
        P(),
        P(),
        P(None, "tensor"),
        P("tensor"),
        P("tensor", None),
    )
    return jax.shard_map(shards, mesh=mesh, in_specs=in_specs, out_specs=out_specs, check_vma=False)
```

```python
import jax
import jax.numpy as jnp
from jax import lax
from jax.sharding import PartitionSpec as P


HD = 64
SLOT = 512

norm_epsilon = 1e-12
big_negative = -1e30
low = jnp.bfloat16
wide = jnp.float32


def bits_of(size):
    return [1 << place for place in range(size.bit_length() - 1)]


def swap(value, axis, bit):
    size = lax.axis_size(axis)
    return lax.ppermute(value, axis, [(index, index ^ bit) for index in range(size)])


def upper(axis, bit):
    return (lax.axis_index(axis) & bit) != 0


def norm_parts(resid):
    center = resid - jnp.mean(resid, axis=-1, keepdims=True)
    scale = lax.rsqrt(jnp.mean(center * center, axis=-1, keepdims=True) + norm_epsilon)
    return center * scale, scale


def norm_back(unit, scale, gain, grad):
    scaled = grad * gain
    back = scale * (
        scaled
        - jnp.mean(scaled, axis=-1, keepdims=True)
        - unit * jnp.mean(scaled * unit, axis=-1, keepdims=True)
    )
    return back, jnp.sum(grad * unit, axis=0), jnp.sum(grad, axis=0)


def gelu_pair(value):
    phi_sum = 0.5 * (1.0 + lax.erf(value * 0.7071067811865476))
    density = jnp.exp(-0.5 * value * value) * 0.3989422804014327
    return value * phi_sum, phi_sum + value * density


def matmul(left, right):
    return jnp.dot(left, right, preferred_element_type=wide)


def matmul_nt(left, right):
    return lax.dot_general(left, right, (((1,), (1,)), ((), ())), preferred_element_type=wide)


def matmul_tn(left, right):
    return lax.dot_general(left, right, (((0,), (0,)), ((), ())), preferred_element_type=wide)


def heads_of(rows):
    return rows.reshape(rows.shape[0], -1, HD)


def attend(query, keys, values, allowed):
    scores = jnp.einsum(
        "qhd,khd->hqk", heads_of(query), heads_of(keys), preferred_element_type=wide
    ) * HD ** (-0.5)
    scores = jnp.where(allowed[None], scores, big_negative)
    row_max = jnp.max(scores, axis=-1, keepdims=True)
    exponent = jnp.exp(scores - row_max)
    total = jnp.sum(exponent, axis=-1, keepdims=True)
    probs = (exponent / total).astype(low)
    context = jnp.einsum("hqk,khd->qhd", probs, heads_of(values), preferred_element_type=wide)
    return context.astype(low).reshape(query.shape), row_max + jnp.log(total)


def attend_back(query, keys, values, grad, log_total, allowed):
    scores = jnp.einsum(
        "qhd,khd->hqk", heads_of(query), heads_of(keys), preferred_element_type=wide
    ) * HD ** (-0.5)
    scores = jnp.where(allowed[None], scores, big_negative)
    probs = jnp.exp(scores - log_total)
    grad_heads = heads_of(grad)
    grad_probs = jnp.einsum(
        "qhd,khd->hqk", grad_heads, heads_of(values), preferred_element_type=wide
    )
    grad_value = jnp.einsum(
        "hqk,qhd->khd", probs.astype(low), grad_heads, preferred_element_type=wide
    )
    inner = jnp.sum(probs * grad_probs, axis=-1, keepdims=True)
    grad_scores = (probs * (grad_probs - inner)).astype(low)
    grad_query = jnp.einsum(
        "hqk,khd->qhd", grad_scores, heads_of(keys), preferred_element_type=wide
    ) * HD ** (-0.5)
    grad_key = jnp.einsum(
        "hqk,qhd->khd", grad_scores, heads_of(query), preferred_element_type=wide
    ) * HD ** (-0.5)
    return [part.astype(low).reshape(query.shape) for part in (grad_query, grad_key, grad_value)]


def gate(*values):
    return lax.optimization_barrier(values)


def fetch_far(block, after):
    far = bits_of(lax.axis_size("tensor"))[1]
    half = block.shape[0] // 2
    piece = lax.dynamic_slice_in_dim(block, jnp.where(upper("dp", 1), half, 0), half)
    piece, *after = gate(piece, *after)
    return swap(piece, "tensor", far), after


def spread(mine, other):
    high = upper("dp", 1)
    away = jnp.concatenate([jnp.where(high, other, mine), jnp.where(high, mine, other)], axis=0)
    return away, swap(away, "tensor", bits_of(lax.axis_size("tensor"))[0])


def near_sum(keep, send):
    near = bits_of(lax.axis_size("tensor"))[0]
    return keep + swap(send, "tensor", near).astype(wide)


def far_sum(keep, send):
    far = bits_of(lax.axis_size("tensor"))[1]
    return keep + swap(send, "tensor", far).astype(wide)


def halve(total, bit):
    half = total.shape[0] // 2
    high = upper("dp", bit)
    keep = lax.dynamic_slice_in_dim(total, jnp.where(high, half, 0), half)
    send = lax.dynamic_slice_in_dim(total, jnp.where(high, 0, half), half)
    return keep + swap(send.astype(low), "dp", bit).astype(wide)


def finish(total, start):
    places = bits_of(lax.axis_size("dp"))
    for bit in places[start:]:
        total = halve(total, bit)
    total = total.astype(low)
    for bit in reversed(places):
        other = swap(total, "dp", bit)
        high = upper("dp", bit)
        total = jnp.concatenate(
            [jnp.where(high, other, total), jnp.where(high, total, other)], axis=0
        )
    return total.astype(wide)


def sum_everywhere(value, axis):
    for bit in bits_of(lax.axis_size(axis)):
        value = value + swap(value, axis, bit)
    return value


def shards(
    inputs,
    out_grad,
    offsets,
    key_keep,
    project_weight,
    project_bias,
    output_weight,
    output_bias,
    norm_gains,
    norm_shifts,
    up_weight,
    up_bias,
    down_weight,
):
    width = inputs.shape[1]
    local_width = project_weight.shape[2]
    units = up_weight.shape[1]
    slot = lax.axis_index("tensor")
    ends = lax.dynamic_slice_in_dim(offsets, slot, 1)
    keep_row = lax.dynamic_slice_in_dim(key_keep, slot * SLOT, SLOT)
    position = jnp.arange(SLOT, dtype=jnp.int32)
    segment = (position >= ends[0, 0]).astype(jnp.int32) + (position >= ends[0, 1]).astype(
        jnp.int32
    )
    seg_start = (position == 0) | (position == ends[0, 0]) | (position == ends[0, 1])
    allowed = (segment[:, None] == segment[None, :]) & ((keep_row == 1) | seg_start)[None, :]
    live_mask = (segment < 2).astype(wide)[:, None]
    biases = output_bias.astype(wide)
    gains = norm_gains.astype(wide)
    shifts = norm_shifts.astype(wide)

    own_bias = jnp.concatenate([project_bias.reshape(-1), up_bias])
    lines = -(-own_bias.shape[0] // width)
    bias_rows = jnp.pad(own_bias, (0, 16 * width - own_bias.shape[0])).reshape(16, width)
    attn_block = jnp.concatenate(
        [project_weight.reshape(width, 3 * local_width).T, output_weight, bias_rows], axis=0
    )
    near, far = bits_of(lax.axis_size("tensor"))
    attn_near = swap(attn_block, "tensor", near)
    attn_far, _ = fetch_far(attn_block, ())
    up_far, (attn_far,) = fetch_far(up_weight, (attn_far,))
    attn_other = swap(attn_far, "dp", 1)
    up_near = swap(up_weight, "tensor", near)
    down_near = swap(down_weight, "tensor", near)
    attn_parts = [attn_block, attn_near]
    edge = 3 * local_width + output_weight.shape[0]
    count = 4

    def bias_of(part):
        return attn_parts[part][edge : edge + lines].reshape(-1)

    saved = []
    attended = 0.0
    for part in range(count):
        if part == 2:
            attended, attn_other = gate(attended, attn_other)
            attn_parts += spread(attn_far, attn_other)
        if part == 3:
            down_far, (up_far, attended) = fetch_far(down_weight, (up_far, attended))
            up_other = swap(up_far, "dp", 1)
        bias = bias_of(part).astype(wide)
        rows = matmul_nt(inputs, attn_parts[part][: 3 * local_width])
        query = (rows[:, :local_width] + bias[:local_width]).astype(low)
        keys = rows[:, local_width : 2 * local_width].astype(low)
        values = (rows[:, 2 * local_width :] + bias[local_width : 2 * local_width]).astype(low)
        context, log_total = attend(query, keys, values, allowed)
        attended = attended + matmul(context, attn_parts[part][3 * local_width : edge])
        saved.append((query, keys, values, context, log_total))

    up_other, down_far, attended = gate(up_other, down_far, attended)
    up_parts = [up_weight, up_near, *spread(up_far, up_other)]
    down_parts = [down_weight, down_near]
    down_other = swap(down_far, "dp", 1)
    resid_one = inputs.astype(wide) + attended + biases[0]
    unit_one, scale_one = norm_parts(resid_one)
    normed_one = unit_one * gains[0] + shifts[0]
    normed_low = normed_one.astype(low)
    ffn_out = 0.0
    kept = []
    for part in range(count):
        if part == 2:
            down_other, ffn_out = gate(down_other, ffn_out)
            down_parts += spread(down_far, down_other)
        bias = bias_of(part)[2 * local_width : 2 * local_width + units].astype(wide)
        active, slope = gelu_pair(matmul(normed_low, up_parts[part]) + bias)
        active = active.astype(low)
        ffn_out = ffn_out + matmul(active, down_parts[part])
        kept.append((active, slope))
    resid_two = normed_one + ffn_out + biases[1]
    unit_two, scale_two = norm_parts(resid_two)
    layer_output = ((unit_two * gains[1] + shifts[1]) * live_mask).astype(low)

    grad_out = out_grad.astype(wide) * live_mask
    grad_two, gain_two, shift_two = norm_back(unit_two, scale_two, gains[1], grad_out)
    grad_ffn = grad_two.astype(low)
    down_grads = [matmul_tn(kept[part][0], grad_ffn) for part in range(count)]
    down_three, down_one, grad_ffn = gate(
        down_grads[3].astype(low), down_grads[1].astype(low), grad_ffn
    )
    down_far_sum = near_sum(down_grads[2], down_three)
    down_total = near_sum(down_grads[0], down_one)
    grad_one_in = grad_two
    grad_pres = []
    for part in range(count):
        grad_act = matmul_nt(grad_ffn, down_parts[part])
        grad_pre = (grad_act * kept[part][1]).astype(low)
        grad_pres.append(grad_pre)
        grad_one_in = grad_one_in + matmul_nt(grad_pre, up_parts[part])
    down_far_low, grad_one_in, down_total = gate(
        down_far_sum.astype(low), grad_one_in, down_total
    )
    down_total = far_sum(down_total, down_far_low)
    up_grads = [matmul_tn(normed_low, grad_pres[part]) for part in range(count)]
    up_three, up_one, grad_one_in = gate(
        up_grads[3].astype(low), up_grads[1].astype(low), grad_one_in
    )
    up_far_sum = near_sum(up_grads[2], up_three)
    up_total = near_sum(up_grads[0], up_one)
    up_bias_grads = [jnp.sum(grad_pres[part], axis=0, dtype=wide) for part in range(count)]

    grad_one, gain_one, shift_one = norm_back(unit_one, scale_one, gains[0], grad_one_in)
    grad_attended = grad_one.astype(low)
    grad_input = 0.0
    attn_grads = {}
    project_bias_grads = {}
    for part in (3, 2, 1, 0):
        query, keys, values, context, log_total = saved[part]
        grad_context = matmul_nt(
            grad_attended, attn_parts[part][3 * local_width : edge]
        ).astype(low)
        pieces = attend_back(query, keys, values, grad_context, log_total, allowed)
        grad_rows = jnp.concatenate(pieces, axis=1)
        grad_input = grad_input + matmul(grad_rows, attn_parts[part][: 3 * local_width])
        attn_grads[part] = jnp.concatenate(
            [matmul_tn(grad_rows, inputs), matmul_tn(context, grad_attended)], axis=0
        )
        project_bias_grads[part] = jnp.concatenate(
            [jnp.sum(pieces[0], axis=0, dtype=wide), jnp.sum(pieces[2], axis=0, dtype=wide)]
        )
        if part == 3:
            attn_three, up_far_low, up_total, down_total, grad_attended = gate(
                attn_grads[3].astype(low),
                up_far_sum.astype(low),
                up_total,
                down_total,
                grad_attended,
            )
            up_total = far_sum(up_total, up_far_low)
            down_total = halve(down_total, 1)
        elif part == 2:
            attn_far_sum = near_sum(attn_grads[2], attn_three)
            attn_far_low, down_total, grad_attended = gate(
                attn_far_sum.astype(low), down_total, grad_attended
            )
            attn_recv = swap(attn_far_low, "tensor", far)
        elif part == 1:
            attn_one, up_total, grad_attended = gate(
                attn_grads[1].astype(low), up_total, grad_attended
            )
            up_total = halve(up_total, 1)
    attn_total = near_sum(attn_grads[0], attn_one)
    attn_recv, grad_input, attn_total = gate(attn_recv, grad_input, attn_total)
    attn_total = attn_total + attn_recv.astype(wide)
    input_grad = (grad_one + grad_input).astype(low)
    down_weight_grad = finish(down_total, 1)
    up_weight_grad = finish(up_total, 1)
    attn_grad = finish(attn_total, 0)
    project_weight_grad = attn_grad[: 3 * local_width].T.reshape(width, 3, local_width)
    output_weight_grad = attn_grad[3 * local_width :]

    small = [
        jnp.concatenate([project_bias_grads[part], up_bias_grads[part]]) for part in range(count)
    ]
    shared = jnp.concatenate(
        [
            jnp.sum(grad_one, axis=0),
            jnp.sum(grad_two, axis=0),
            gain_one,
            gain_two,
            shift_one,
            shift_two,
        ]
    )
    length = small[0].shape[0]
    small_send, grad_input = gate(jnp.concatenate([small[1], small[3], shared]), grad_input)
    from_near = swap(small_send, "tensor", near)
    pair = jnp.concatenate([small[0], small[2], shared]) + from_near
    from_far = swap(pair[length:], "tensor", far)
    packed = jnp.concatenate(
        [pair[:length] + from_far[:length], pair[2 * length :] + from_far[length:]]
    )
    packed = sum_everywhere(packed, "dp")
    project_bias_grad = packed[: 2 * local_width].reshape(2, local_width)
    up_bias_grad = packed[2 * local_width : length]
    norm_grads = packed[length:].reshape(3, 2, width)
    return (
        layer_output,
        input_grad,
        project_weight_grad,
        project_bias_grad,
        output_weight_grad,
        norm_grads[0],
        norm_grads[1],
        norm_grads[2],
        up_weight_grad,
        up_bias_grad,
        down_weight_grad,
    )


def solution(mesh):
    in_specs = (
        P(("dp", "tensor"), None),
        P(("dp", "tensor"), None),
        P("dp", None),
        P("dp"),
        P(None, None, "tensor"),
        P(None, "tensor"),
        P("tensor", None),
        P(),
        P(),
        P(),
        P(None, "tensor"),
        P("tensor"),
        P("tensor", None),
    )
    out_specs = (
        P(("dp", "tensor"), None),
        P(("dp", "tensor"), None),
        P(None, None, "tensor"),
        P(None, "tensor"),
        P("tensor", None),
        P(),
        P(),
        P(),
        P(None, "tensor"),
        P("tensor"),
        P("tensor", None),
    )

    return jax.shard_map(shards, mesh=mesh, in_specs=in_specs, out_specs=out_specs, check_vma=False)
```

```python
import jax
import jax.numpy as jnp
from jax import lax
from jax.sharding import PartitionSpec as P


HD = 64
SLOT = 512

norm_epsilon = 1e-12
big_negative = -1e30
low = jnp.bfloat16
wide = jnp.float32


def bits_of(size):
    return [1 << place for place in range(size.bit_length() - 1)]


def swap(value, axis, bit):
    size = lax.axis_size(axis)
    return lax.ppermute(value, axis, [(index, index ^ bit) for index in range(size)])


def upper(axis, bit):
    return (lax.axis_index(axis) & bit) != 0


def norm_parts(resid):
    center = resid - jnp.mean(resid, axis=-1, keepdims=True)
    scale = lax.rsqrt(jnp.mean(center * center, axis=-1, keepdims=True) + norm_epsilon)
    return center * scale, scale


def norm_back(unit, scale, gain, grad):
    scaled = grad * gain
    back = scale * (
        scaled
        - jnp.mean(scaled, axis=-1, keepdims=True)
        - unit * jnp.mean(scaled * unit, axis=-1, keepdims=True)
    )
    return back, jnp.sum(grad * unit, axis=0), jnp.sum(grad, axis=0)


def gelu_pair(value):
    phi_sum = 0.5 * (1.0 + lax.erf(value * 0.7071067811865476))
    density = jnp.exp(-0.5 * value * value) * 0.3989422804014327
    return value * phi_sum, phi_sum + value * density


def matmul(left, right):
    return jnp.dot(left, right, preferred_element_type=wide)


def matmul_nt(left, right):
    return lax.dot_general(left, right, (((1,), (1,)), ((), ())), preferred_element_type=wide)


def matmul_tn(left, right):
    return lax.dot_general(left, right, (((0,), (0,)), ((), ())), preferred_element_type=wide)


def heads_of(rows):
    return rows.reshape(rows.shape[0], -1, HD)


def attend(query, keys, values, allowed):
    scores = jnp.einsum(
        "qhd,khd->hqk", heads_of(query), heads_of(keys), preferred_element_type=wide
    ) * HD ** (-0.5)
    scores = jnp.where(allowed[None], scores, big_negative)
    row_max = jnp.max(scores, axis=-1, keepdims=True)
    exponent = jnp.exp(scores - row_max)
    total = jnp.sum(exponent, axis=-1, keepdims=True)
    probs = (exponent / total).astype(low)
    context = jnp.einsum("hqk,khd->qhd", probs, heads_of(values), preferred_element_type=wide)
    return context.astype(low).reshape(query.shape), row_max + jnp.log(total)


def attend_back(query, keys, values, grad, log_total, allowed):
    scores = jnp.einsum(
        "qhd,khd->hqk", heads_of(query), heads_of(keys), preferred_element_type=wide
    ) * HD ** (-0.5)
    scores = jnp.where(allowed[None], scores, big_negative)
    probs = jnp.exp(scores - log_total)
    grad_heads = heads_of(grad)
    grad_probs = jnp.einsum(
        "qhd,khd->hqk", grad_heads, heads_of(values), preferred_element_type=wide
    )
    grad_value = jnp.einsum(
        "hqk,qhd->khd", probs.astype(low), grad_heads, preferred_element_type=wide
    )
    inner = jnp.sum(probs * grad_probs, axis=-1, keepdims=True)
    grad_scores = (probs * (grad_probs - inner)).astype(low)
    grad_query = jnp.einsum(
        "hqk,khd->qhd", grad_scores, heads_of(keys), preferred_element_type=wide
    ) * HD ** (-0.5)
    grad_key = jnp.einsum(
        "hqk,qhd->khd", grad_scores, heads_of(query), preferred_element_type=wide
    ) * HD ** (-0.5)
    return [part.astype(low).reshape(query.shape) for part in (grad_query, grad_key, grad_value)]


def gate(*values):
    return lax.optimization_barrier(values)


def fetch_far(block, after):
    far = bits_of(lax.axis_size("tensor"))[1]
    half = block.shape[0] // 2
    piece = lax.dynamic_slice_in_dim(block, jnp.where(upper("dp", 1), half, 0), half)
    piece, *after = gate(piece, *after)
    return swap(piece, "tensor", far), after


def spread(mine, other):
    high = upper("dp", 1)
    away = jnp.concatenate([jnp.where(high, other, mine), jnp.where(high, mine, other)], axis=0)
    return away, swap(away, "tensor", bits_of(lax.axis_size("tensor"))[0])


def near_sum(keep, send):
    near = bits_of(lax.axis_size("tensor"))[0]
    return keep + swap(send, "tensor", near).astype(wide)


def far_sum(keep, send):
    far = bits_of(lax.axis_size("tensor"))[1]
    return keep + swap(send, "tensor", far).astype(wide)


def halve(total, bit):
    half = total.shape[0] // 2
    high = upper("dp", bit)
    keep = lax.dynamic_slice_in_dim(total, jnp.where(high, half, 0), half)
    send = lax.dynamic_slice_in_dim(total, jnp.where(high, 0, half), half)
    return keep + swap(send.astype(low), "dp", bit).astype(wide)


def finish(total, start):
    places = bits_of(lax.axis_size("dp"))
    for bit in places[start:]:
        total = halve(total, bit)
    total = total.astype(low)
    for bit in reversed(places):
        other = swap(total, "dp", bit)
        high = upper("dp", bit)
        total = jnp.concatenate(
            [jnp.where(high, other, total), jnp.where(high, total, other)], axis=0
        )
    return total.astype(wide)


def shards(
    inputs,
    out_grad,
    offsets,
    key_keep,
    project_weight,
    project_bias,
    output_weight,
    output_bias,
    norm_gains,
    norm_shifts,
    up_weight,
    up_bias,
    down_weight,
):
    width = inputs.shape[1]
    local_width = project_weight.shape[2]
    units = up_weight.shape[1]
    slot = lax.axis_index("tensor")
    ends = lax.dynamic_slice_in_dim(offsets, slot, 1)
    keep_row = lax.dynamic_slice_in_dim(key_keep, slot * SLOT, SLOT)
    position = jnp.arange(SLOT, dtype=jnp.int32)
    segment = (position >= ends[0, 0]).astype(jnp.int32) + (position >= ends[0, 1]).astype(
        jnp.int32
    )
    seg_start = (position == 0) | (position == ends[0, 0]) | (position == ends[0, 1])
    allowed = (segment[:, None] == segment[None, :]) & ((keep_row == 1) | seg_start)[None, :]
    live_mask = (segment < 2).astype(wide)[:, None]
    biases = output_bias.astype(wide)
    gains = norm_gains.astype(wide)
    shifts = norm_shifts.astype(wide)

    own_bias = jnp.concatenate([project_bias.reshape(-1), up_bias])
    lines = -(-own_bias.shape[0] // width)
    bias_rows = jnp.pad(own_bias, (0, 16 * width - own_bias.shape[0])).reshape(16, width)
    attn_block = jnp.concatenate(
        [project_weight.reshape(width, 3 * local_width).T, output_weight, bias_rows], axis=0
    )
    near, far = bits_of(lax.axis_size("tensor"))
    attn_near = swap(attn_block, "tensor", near)
    attn_far, _ = fetch_far(attn_block, ())
    up_far, (attn_far,) = fetch_far(up_weight, (attn_far,))
    attn_other = swap(attn_far, "dp", 1)
    up_near = swap(up_weight, "tensor", near)
    down_near = swap(down_weight, "tensor", near)
    attn_parts = [attn_block, attn_near]
    edge = 3 * local_width + output_weight.shape[0]
    count = 4

    def bias_of(part):
        return attn_parts[part][edge : edge + lines].reshape(-1)

    saved = []
    attended = 0.0
    for part in range(count):
        if part == 2:
            attended, attn_other = gate(attended, attn_other)
            attn_parts += spread(attn_far, attn_other)
        if part == 3:
            down_far, (up_far, attended) = fetch_far(down_weight, (up_far, attended))
            up_other = swap(up_far, "dp", 1)
        bias = bias_of(part).astype(wide)
        rows = matmul_nt(inputs, attn_parts[part][: 3 * local_width])
        query = (rows[:, :local_width] + bias[:local_width]).astype(low)
        keys = rows[:, local_width : 2 * local_width].astype(low)
        values = (rows[:, 2 * local_width :] + bias[local_width : 2 * local_width]).astype(low)
        context, log_total = attend(query, keys, values, allowed)
        attended = attended + matmul(context, attn_parts[part][3 * local_width : edge])
        saved.append((query, keys, values, context, log_total))

    up_other, down_far, attended = gate(up_other, down_far, attended)
    up_parts = [up_weight, up_near, *spread(up_far, up_other)]
    down_parts = [down_weight, down_near]
    down_other = swap(down_far, "dp", 1)
    resid_one = inputs.astype(wide) + attended + biases[0]
    unit_one, scale_one = norm_parts(resid_one)
    normed_one = unit_one * gains[0] + shifts[0]
    normed_low = normed_one.astype(low)
    ffn_out = 0.0
    kept = []
    for part in range(count):
        if part == 2:
            down_other, ffn_out = gate(down_other, ffn_out)
            down_parts += spread(down_far, down_other)
        bias = bias_of(part)[2 * local_width : 2 * local_width + units].astype(wide)
        active, slope = gelu_pair(matmul(normed_low, up_parts[part]) + bias)
        active = active.astype(low)
        ffn_out = ffn_out + matmul(active, down_parts[part])
        kept.append((active, slope))
    resid_two = normed_one + ffn_out + biases[1]
    unit_two, scale_two = norm_parts(resid_two)
    layer_output = ((unit_two * gains[1] + shifts[1]) * live_mask).astype(low)

    grad_out = out_grad.astype(wide) * live_mask
    grad_two, gain_two, shift_two = norm_back(unit_two, scale_two, gains[1], grad_out)
    grad_ffn = grad_two.astype(low)
    down_grads = [matmul_tn(kept[part][0], grad_ffn) for part in range(count)]
    down_three, down_one, grad_ffn = gate(
        down_grads[3].astype(low), down_grads[1].astype(low), grad_ffn
    )
    down_far_sum = near_sum(down_grads[2], down_three)
    down_total = near_sum(down_grads[0], down_one)
    grad_one_in = grad_two
    grad_pres = []
    for part in range(count):
        grad_act = matmul_nt(grad_ffn, down_parts[part])
        grad_pre = (grad_act * kept[part][1]).astype(low)
        grad_pres.append(grad_pre)
        grad_one_in = grad_one_in + matmul_nt(grad_pre, up_parts[part])
    down_far_low, grad_one_in, down_total = gate(
        down_far_sum.astype(low), grad_one_in, down_total
    )
    down_total = far_sum(down_total, down_far_low)
    up_grads = [matmul_tn(normed_low, grad_pres[part]) for part in range(count)]
    up_three, up_one, grad_one_in = gate(
        up_grads[3].astype(low), up_grads[1].astype(low), grad_one_in
    )
    up_far_sum = near_sum(up_grads[2], up_three)
    up_total = near_sum(up_grads[0], up_one)
    up_bias_grads = [jnp.sum(grad_pres[part], axis=0, dtype=wide) for part in range(count)]

    grad_one, gain_one, shift_one = norm_back(unit_one, scale_one, gains[0], grad_one_in)
    grad_attended = grad_one.astype(low)
    grad_input = 0.0
    extra = 8 * lax.axis_size("dp")
    attn_grads = {}
    shared = jnp.concatenate(
        [
            jnp.sum(grad_one, axis=0),
            jnp.sum(grad_two, axis=0),
            gain_one,
            gain_two,
            shift_one,
            shift_two,
        ]
    ).reshape(-1, width)
    for part in (3, 2, 1, 0):
        query, keys, values, context, log_total = saved[part]
        grad_context = matmul_nt(
            grad_attended, attn_parts[part][3 * local_width : edge]
        ).astype(low)
        pieces = attend_back(query, keys, values, grad_context, log_total, allowed)
        grad_rows = jnp.concatenate(pieces, axis=1)
        grad_input = grad_input + matmul(grad_rows, attn_parts[part][: 3 * local_width])
        own_small = jnp.concatenate(
            [
                jnp.sum(pieces[0], axis=0, dtype=wide),
                jnp.sum(pieces[2], axis=0, dtype=wide),
                up_bias_grads[part],
            ]
        )
        own_rows = jnp.pad(
            own_small, (0, (extra - shared.shape[0]) * width - own_small.shape[0])
        ).reshape(-1, width)
        attn_grads[part] = jnp.concatenate(
            [
                matmul_tn(grad_rows, inputs),
                matmul_tn(context, grad_attended),
                shared,
                own_rows,
            ],
            axis=0,
        )
        if part == 3:
            attn_three, up_far_low, up_total, down_total, grad_attended = gate(
                attn_grads[3].astype(low),
                up_far_sum.astype(low),
                up_total,
                down_total,
                grad_attended,
            )
            up_total = far_sum(up_total, up_far_low)
            down_total = halve(down_total, 1)
        elif part == 2:
            attn_far_sum = near_sum(attn_grads[2], attn_three)
            attn_far_low, down_total, grad_attended = gate(
                attn_far_sum.astype(low), down_total, grad_attended
            )
            attn_recv = swap(attn_far_low, "tensor", far)
        elif part == 1:
            attn_one, up_total, grad_attended = gate(
                attn_grads[1].astype(low), up_total, grad_attended
            )
            up_total = halve(up_total, 1)
    attn_total = near_sum(attn_grads[0], attn_one)
    attn_recv, grad_input, attn_total, up_total, down_total = gate(
        attn_recv, grad_input, attn_total, up_total, down_total
    )
    attn_total = attn_total + attn_recv.astype(wide)
    attn_grad = finish(attn_total, 0)
    up_weight_grad = finish(up_total, 1)
    down_weight_grad = finish(down_total, 1)
    input_grad = (grad_one + grad_input).astype(low)
    project_weight_grad = attn_grad[: 3 * local_width].T.reshape(width, 3, local_width)
    output_weight_grad = attn_grad[3 * local_width : edge]
    lower = edge + shared.shape[0]
    norm_grads = attn_grad[edge:lower].reshape(3, 2, width)
    own_small = attn_grad[lower : lower + lines].reshape(-1)
    project_bias_grad = own_small[: 2 * local_width].reshape(2, local_width)
    up_bias_grad = own_small[2 * local_width : 2 * local_width + units]
    return (
        layer_output,
        input_grad,
        project_weight_grad,
        project_bias_grad,
        output_weight_grad,
        norm_grads[0],
        norm_grads[1],
        norm_grads[2],
        up_weight_grad,
        up_bias_grad,
        down_weight_grad,
    )


def solution(mesh):
    in_specs = (
        P(("dp", "tensor"), None),
        P(("dp", "tensor"), None),
        P("dp", None),
        P("dp"),
        P(None, None, "tensor"),
        P(None, "tensor"),
        P("tensor", None),
        P(),
        P(),
        P(),
        P(None, "tensor"),
        P("tensor"),
        P("tensor", None),
    )
    out_specs = (
        P(("dp", "tensor"), None),
        P(("dp", "tensor"), None),
        P(None, None, "tensor"),
        P(None, "tensor"),
        P("tensor", None),
        P(),
        P(),
        P(),
        P(None, "tensor"),
        P("tensor"),
        P("tensor", None),
    )

    return jax.shard_map(shards, mesh=mesh, in_specs=in_specs, out_specs=out_specs, check_vma=False)
```

```python
import jax
import jax.numpy as jnp
from jax import lax
from jax.sharding import PartitionSpec as P


HD = 64
SLOT = 512

norm_epsilon = 1e-12
big_negative = -1e30
low = jnp.bfloat16
wide = jnp.float32


def bits_of(size):
    return [1 << place for place in range(size.bit_length() - 1)]


def swap(value, axis, bit):
    size = lax.axis_size(axis)
    return lax.ppermute(value, axis, [(index, index ^ bit) for index in range(size)])


def upper(axis, bit):
    return (lax.axis_index(axis) & bit) != 0


def norm_parts(resid):
    center = resid - jnp.mean(resid, axis=-1, keepdims=True)
    scale = lax.rsqrt(jnp.mean(center * center, axis=-1, keepdims=True) + norm_epsilon)
    return center * scale, scale


def norm_back(unit, scale, gain, grad):
    scaled = grad * gain
    back = scale * (
        scaled
        - jnp.mean(scaled, axis=-1, keepdims=True)
        - unit * jnp.mean(scaled * unit, axis=-1, keepdims=True)
    )
    return back, jnp.sum(grad * unit, axis=0), jnp.sum(grad, axis=0)


def gelu_pair(value):
    phi_sum = 0.5 * (1.0 + lax.erf(value * 0.7071067811865476))
    density = jnp.exp(-0.5 * value * value) * 0.3989422804014327
    return value * phi_sum, phi_sum + value * density


def matmul(left, right):
    return jnp.dot(left, right, preferred_element_type=wide)


def matmul_nt(left, right):
    return lax.dot_general(left, right, (((1,), (1,)), ((), ())), preferred_element_type=wide)


def matmul_tn(left, right):
    return lax.dot_general(left, right, (((0,), (0,)), ((), ())), preferred_element_type=wide)


def heads_of(rows):
    return rows.reshape(rows.shape[0], -1, HD)


def attend(query, keys, values, allowed):
    scores = jnp.einsum(
        "qhd,khd->hqk", heads_of(query), heads_of(keys), preferred_element_type=wide
    ) * HD ** (-0.5)
    scores = jnp.where(allowed[None], scores, big_negative)
    row_max = jnp.max(scores, axis=-1, keepdims=True)
    exponent = jnp.exp(scores - row_max)
    total = jnp.sum(exponent, axis=-1, keepdims=True)
    probs = (exponent / total).astype(low)
    context = jnp.einsum("hqk,khd->qhd", probs, heads_of(values), preferred_element_type=wide)
    return context.astype(low).reshape(query.shape), row_max + jnp.log(total)


def attend_back(query, keys, values, grad, log_total, allowed):
    scores = jnp.einsum(
        "qhd,khd->hqk", heads_of(query), heads_of(keys), preferred_element_type=wide
    ) * HD ** (-0.5)
    scores = jnp.where(allowed[None], scores, big_negative)
    probs = jnp.exp(scores - log_total)
    grad_heads = heads_of(grad)
    grad_probs = jnp.einsum(
        "qhd,khd->hqk", grad_heads, heads_of(values), preferred_element_type=wide
    )
    grad_value = jnp.einsum(
        "hqk,qhd->khd", probs.astype(low), grad_heads, preferred_element_type=wide
    )
    inner = jnp.sum(probs * grad_probs, axis=-1, keepdims=True)
    grad_scores = (probs * (grad_probs - inner)).astype(low)
    grad_query = jnp.einsum(
        "hqk,khd->qhd", grad_scores, heads_of(keys), preferred_element_type=wide
    ) * HD ** (-0.5)
    grad_key = jnp.einsum(
        "hqk,qhd->khd", grad_scores, heads_of(query), preferred_element_type=wide
    ) * HD ** (-0.5)
    return [part.astype(low).reshape(query.shape) for part in (grad_query, grad_key, grad_value)]


def gate(*values):
    return lax.optimization_barrier(values)


def fetch_far(block, after):
    far = bits_of(lax.axis_size("tensor"))[1]
    half = block.shape[0] // 2
    piece = lax.dynamic_slice_in_dim(block, jnp.where(upper("dp", 1), half, 0), half)
    piece, *after = gate(piece, *after)
    return swap(piece, "tensor", far), after


def spread(mine, other):
    high = upper("dp", 1)
    away = jnp.concatenate([jnp.where(high, other, mine), jnp.where(high, mine, other)], axis=0)
    return away, swap(away, "tensor", bits_of(lax.axis_size("tensor"))[0])


def near_sum(keep, send):
    near = bits_of(lax.axis_size("tensor"))[0]
    return keep + swap(send, "tensor", near).astype(wide)


def halve(total, bit):
    half = total.shape[0] // 2
    high = upper("dp", bit)
    keep = lax.dynamic_slice_in_dim(total, jnp.where(high, half, 0), half)
    send = lax.dynamic_slice_in_dim(total, jnp.where(high, 0, half), half)
    return keep + swap(send.astype(low), "dp", bit).astype(wide)


def finish(total, start):
    places = bits_of(lax.axis_size("dp"))
    for bit in places[start:]:
        total = halve(total, bit)
    total = total.astype(low)
    for bit in reversed(places):
        other = swap(total, "dp", bit)
        high = upper("dp", bit)
        total = jnp.concatenate(
            [jnp.where(high, other, total), jnp.where(high, total, other)], axis=0
        )
    return total.astype(wide)


def shards(
    inputs,
    out_grad,
    offsets,
    key_keep,
    project_weight,
    project_bias,
    output_weight,
    output_bias,
    norm_gains,
    norm_shifts,
    up_weight,
    up_bias,
    down_weight,
):
    width = inputs.shape[1]
    local_width = project_weight.shape[2]
    units = up_weight.shape[1]
    slot = lax.axis_index("tensor")
    ends = lax.dynamic_slice_in_dim(offsets, slot, 1)
    keep_row = lax.dynamic_slice_in_dim(key_keep, slot * SLOT, SLOT)
    position = jnp.arange(SLOT, dtype=jnp.int32)
    segment = (position >= ends[0, 0]).astype(jnp.int32) + (position >= ends[0, 1]).astype(
        jnp.int32
    )
    seg_start = (position == 0) | (position == ends[0, 0]) | (position == ends[0, 1])
    allowed = (segment[:, None] == segment[None, :]) & ((keep_row == 1) | seg_start)[None, :]
    live_mask = (segment < 2).astype(wide)[:, None]
    biases = output_bias.astype(wide)
    gains = norm_gains.astype(wide)
    shifts = norm_shifts.astype(wide)

    own_bias = jnp.concatenate([project_bias.reshape(-1), up_bias])
    lines = -(-own_bias.shape[0] // width)
    bias_rows = jnp.pad(own_bias, (0, 16 * width - own_bias.shape[0])).reshape(16, width)
    attn_block = jnp.concatenate(
        [project_weight.reshape(width, 3 * local_width).T, output_weight, bias_rows], axis=0
    )
    near, far = bits_of(lax.axis_size("tensor"))
    attn_near = swap(attn_block, "tensor", near)
    attn_far, _ = fetch_far(attn_block, ())
    up_far, (attn_far,) = fetch_far(up_weight, (attn_far,))
    attn_other = swap(attn_far, "dp", 1)
    up_near = swap(up_weight, "tensor", near)
    down_near = swap(down_weight, "tensor", near)
    attn_parts = [attn_block, attn_near]
    edge = 3 * local_width + output_weight.shape[0]
    count = 4

    def bias_of(part):
        return attn_parts[part][edge : edge + lines].reshape(-1)

    saved = []
    attended = 0.0
    for part in range(count):
        if part == 2:
            attended, attn_other = gate(attended, attn_other)
            attn_parts += spread(attn_far, attn_other)
        if part == 3:
            down_far, (up_far, attended) = fetch_far(down_weight, (up_far, attended))
            up_other = swap(up_far, "dp", 1)
        bias = bias_of(part).astype(wide)
        rows = matmul_nt(inputs, attn_parts[part][: 3 * local_width])
        query = (rows[:, :local_width] + bias[:local_width]).astype(low)
        keys = rows[:, local_width : 2 * local_width].astype(low)
        values = (rows[:, 2 * local_width :] + bias[local_width : 2 * local_width]).astype(low)
        context, log_total = attend(query, keys, values, allowed)
        attended = attended + matmul(context, attn_parts[part][3 * local_width : edge])
        saved.append((query, keys, values, context, log_total))

    up_other, down_far, attended = gate(up_other, down_far, attended)
    up_parts = [up_weight, up_near, *spread(up_far, up_other)]
    down_parts = [down_weight, down_near]
    down_other = swap(down_far, "dp", 1)
    resid_one = inputs.astype(wide) + attended + biases[0]
    unit_one, scale_one = norm_parts(resid_one)
    normed_one = unit_one * gains[0] + shifts[0]
    normed_low = normed_one.astype(low)
    ffn_out = 0.0
    kept = []
    for part in range(count):
        if part == 2:
            down_other, ffn_out = gate(down_other, ffn_out)
            down_parts += spread(down_far, down_other)
        bias = bias_of(part)[2 * local_width : 2 * local_width + units].astype(wide)
        active, slope = gelu_pair(matmul(normed_low, up_parts[part]) + bias)
        active = active.astype(low)
        ffn_out = ffn_out + matmul(active, down_parts[part])
        kept.append((active, slope))
    resid_two = normed_one + ffn_out + biases[1]
    unit_two, scale_two = norm_parts(resid_two)
    layer_output = ((unit_two * gains[1] + shifts[1]) * live_mask).astype(low)

    grad_out = out_grad.astype(wide) * live_mask
    grad_two, gain_two, shift_two = norm_back(unit_two, scale_two, gains[1], grad_out)
    grad_ffn = grad_two.astype(low)
    down_grads = [matmul_tn(kept[part][0], grad_ffn) for part in range(count)]
    down_three, down_one, grad_ffn = gate(
        down_grads[3].astype(low), down_grads[1].astype(low), grad_ffn
    )
    down_far_sum = near_sum(down_grads[2], down_three)
    down_total = near_sum(down_grads[0], down_one)
    grad_one_in = grad_two
    grad_pres = []
    for part in range(count):
        grad_act = matmul_nt(grad_ffn, down_parts[part])
        grad_pre = (grad_act * kept[part][1]).astype(low)
        grad_pres.append(grad_pre)
        grad_one_in = grad_one_in + matmul_nt(grad_pre, up_parts[part])
        if part == 1:
            down_far_low, grad_ffn, grad_one_in, down_total = gate(
                down_far_sum.astype(low), grad_ffn, grad_one_in, down_total
            )
            down_recv = swap(down_far_low, "tensor", far)
    up_grads = [matmul_tn(normed_low, grad_pres[part]) for part in range(count)]
    up_three, up_one, grad_one_in = gate(
        up_grads[3].astype(low), up_grads[1].astype(low), grad_one_in
    )
    up_far_low, grad_one_in = gate(
        near_sum(up_grads[2], up_three).astype(low), grad_one_in
    )
    up_recv = swap(up_far_low, "tensor", far)
    up_total = near_sum(up_grads[0], up_one)
    up_bias_grads = [jnp.sum(grad_pres[part], axis=0, dtype=wide) for part in range(count)]

    grad_one, gain_one, shift_one = norm_back(unit_one, scale_one, gains[0], grad_one_in)
    grad_attended = grad_one.astype(low)
    grad_input = 0.0
    extra = 8 * lax.axis_size("dp")
    attn_grads = {}
    shared = jnp.concatenate(
        [
            jnp.sum(grad_one, axis=0),
            jnp.sum(grad_two, axis=0),
            gain_one,
            gain_two,
            shift_one,
            shift_two,
        ]
    ).reshape(-1, width)
    for part in (3, 2, 1, 0):
        query, keys, values, context, log_total = saved[part]
        grad_context = matmul_nt(
            grad_attended, attn_parts[part][3 * local_width : edge]
        ).astype(low)
        pieces = attend_back(query, keys, values, grad_context, log_total, allowed)
        grad_rows = jnp.concatenate(pieces, axis=1)
        grad_input = grad_input + matmul(grad_rows, attn_parts[part][: 3 * local_width])
        own_small = jnp.concatenate(
            [
                jnp.sum(pieces[0], axis=0, dtype=wide),
                jnp.sum(pieces[2], axis=0, dtype=wide),
                up_bias_grads[part],
            ]
        )
        own_rows = jnp.pad(
            own_small, (0, (extra - shared.shape[0]) * width - own_small.shape[0])
        ).reshape(-1, width)
        attn_grads[part] = jnp.concatenate(
            [
                matmul_tn(grad_rows, inputs),
                matmul_tn(context, grad_attended),
                shared,
                own_rows,
            ],
            axis=0,
        )
        if part == 3:
            attn_three, down_recv, down_total, grad_attended = gate(
                attn_grads[3].astype(low), down_recv, down_total, grad_attended
            )
            down_total = halve(down_total + down_recv.astype(wide), 1)
        elif part == 2:
            attn_far_sum = near_sum(attn_grads[2], attn_three)
            attn_far_low, down_total, grad_attended = gate(
                attn_far_sum.astype(low), down_total, grad_attended
            )
            attn_recv = swap(attn_far_low, "tensor", far)
        elif part == 1:
            attn_one, up_recv, up_total, grad_attended = gate(
                attn_grads[1].astype(low), up_recv, up_total, grad_attended
            )
            up_total = halve(up_total + up_recv.astype(wide), 1)
    attn_total = near_sum(attn_grads[0], attn_one)
    attn_recv, grad_input, attn_total, up_total, down_total = gate(
        attn_recv, grad_input, attn_total, up_total, down_total
    )
    attn_total = attn_total + attn_recv.astype(wide)
    attn_grad = finish(attn_total, 0)
    up_weight_grad = finish(up_total, 1)
    down_weight_grad = finish(down_total, 1)
    input_grad = (grad_one + grad_input).astype(low)
    project_weight_grad = attn_grad[: 3 * local_width].T.reshape(width, 3, local_width)
    output_weight_grad = attn_grad[3 * local_width : edge]
    lower = edge + shared.shape[0]
    norm_grads = attn_grad[edge:lower].reshape(3, 2, width)
    own_small = attn_grad[lower : lower + lines].reshape(-1)
    project_bias_grad = own_small[: 2 * local_width].reshape(2, local_width)
    up_bias_grad = own_small[2 * local_width : 2 * local_width + units]
    return (
        layer_output,
        input_grad,
        project_weight_grad,
        project_bias_grad,
        output_weight_grad,
        norm_grads[0],
        norm_grads[1],
        norm_grads[2],
        up_weight_grad,
        up_bias_grad,
        down_weight_grad,
    )


def solution(mesh):
    in_specs = (
        P(("dp", "tensor"), None),
        P(("dp", "tensor"), None),
        P("dp", None),
        P("dp"),
        P(None, None, "tensor"),
        P(None, "tensor"),
        P("tensor", None),
        P(),
        P(),
        P(),
        P(None, "tensor"),
        P("tensor"),
        P("tensor", None),
    )
    out_specs = (
        P(("dp", "tensor"), None),
        P(("dp", "tensor"), None),
        P(None, None, "tensor"),
        P(None, "tensor"),
        P("tensor", None),
        P(),
        P(),
        P(),
        P(None, "tensor"),
        P("tensor"),
        P("tensor", None),
    )

    return jax.shard_map(shards, mesh=mesh, in_specs=in_specs, out_specs=out_specs, check_vma=False)
```

```python
import jax
import jax.numpy as jnp
from jax import lax
from jax.sharding import PartitionSpec as P


HD = 64
SLOT = 512

norm_epsilon = 1e-12
big_negative = -1e30
low = jnp.bfloat16
wide = jnp.float32


def bits_of(size):
    return [1 << place for place in range(size.bit_length() - 1)]


def swap(value, axis, bit):
    size = lax.axis_size(axis)
    return lax.ppermute(value, axis, [(index, index ^ bit) for index in range(size)])


def upper(axis, bit):
    return (lax.axis_index(axis) & bit) != 0


def norm_parts(resid):
    center = resid - jnp.mean(resid, axis=-1, keepdims=True)
    scale = lax.rsqrt(jnp.mean(center * center, axis=-1, keepdims=True) + norm_epsilon)
    return center * scale, scale


def norm_back(unit, scale, gain, grad):
    scaled = grad * gain
    back = scale * (
        scaled
        - jnp.mean(scaled, axis=-1, keepdims=True)
        - unit * jnp.mean(scaled * unit, axis=-1, keepdims=True)
    )
    return back, jnp.sum(grad * unit, axis=0), jnp.sum(grad, axis=0)


def gelu_pair(value):
    phi_sum = 0.5 * (1.0 + lax.erf(value * 0.7071067811865476))
    density = jnp.exp(-0.5 * value * value) * 0.3989422804014327
    return value * phi_sum, phi_sum + value * density


def matmul(left, right):
    return jnp.dot(left, right, preferred_element_type=wide)


def matmul_nt(left, right):
    return lax.dot_general(left, right, (((1,), (1,)), ((), ())), preferred_element_type=wide)


def matmul_tn(left, right):
    return lax.dot_general(left, right, (((0,), (0,)), ((), ())), preferred_element_type=wide)


def heads_of(rows):
    return rows.reshape(rows.shape[0], -1, HD)


def attend(query, keys, values, allowed):
    scores = jnp.einsum(
        "qhd,khd->hqk", heads_of(query), heads_of(keys), preferred_element_type=wide
    ) * HD ** (-0.5)
    scores = jnp.where(allowed[None], scores, big_negative)
    row_max = jnp.max(scores, axis=-1, keepdims=True)
    exponent = jnp.exp(scores - row_max)
    total = jnp.sum(exponent, axis=-1, keepdims=True)
    probs = (exponent / total).astype(low)
    context = jnp.einsum("hqk,khd->qhd", probs, heads_of(values), preferred_element_type=wide)
    return context.astype(low).reshape(query.shape), row_max + jnp.log(total)


def attend_back(query, keys, values, grad, log_total, allowed):
    scores = jnp.einsum(
        "qhd,khd->hqk", heads_of(query), heads_of(keys), preferred_element_type=wide
    ) * HD ** (-0.5)
    scores = jnp.where(allowed[None], scores, big_negative)
    probs = jnp.exp(scores - log_total)
    grad_heads = heads_of(grad)
    grad_probs = jnp.einsum(
        "qhd,khd->hqk", grad_heads, heads_of(values), preferred_element_type=wide
    )
    grad_value = jnp.einsum(
        "hqk,qhd->khd", probs.astype(low), grad_heads, preferred_element_type=wide
    )
    inner = jnp.sum(probs * grad_probs, axis=-1, keepdims=True)
    grad_scores = (probs * (grad_probs - inner)).astype(low)
    grad_query = jnp.einsum(
        "hqk,khd->qhd", grad_scores, heads_of(keys), preferred_element_type=wide
    ) * HD ** (-0.5)
    grad_key = jnp.einsum(
        "hqk,qhd->khd", grad_scores, heads_of(query), preferred_element_type=wide
    ) * HD ** (-0.5)
    return [part.astype(low).reshape(query.shape) for part in (grad_query, grad_key, grad_value)]


def gate(*values):
    return lax.optimization_barrier(values)


def fetch_far(block, after):
    far = bits_of(lax.axis_size("tensor"))[1]
    half = block.shape[0] // 2
    piece = lax.dynamic_slice_in_dim(block, jnp.where(upper("dp", 1), half, 0), half)
    piece, *after = gate(piece, *after)
    return swap(piece, "tensor", far), after


def spread(mine, other):
    high = upper("dp", 1)
    away = jnp.concatenate([jnp.where(high, other, mine), jnp.where(high, mine, other)], axis=0)
    return away, swap(away, "tensor", bits_of(lax.axis_size("tensor"))[0])


def near_sum(keep, send):
    near = bits_of(lax.axis_size("tensor"))[0]
    return keep + swap(send, "tensor", near).astype(wide)


def halve(total, bit):
    half = total.shape[-2] // 2
    high = upper("dp", bit)
    axis = total.ndim - 2
    keep = lax.dynamic_slice_in_dim(total, jnp.where(high, half, 0), half, axis)
    send = lax.dynamic_slice_in_dim(total, jnp.where(high, 0, half), half, axis)
    return keep + swap(send.astype(low), "dp", bit).astype(wide)


def finish(total, start):
    places = bits_of(lax.axis_size("dp"))
    for bit in places[start:]:
        total = halve(total, bit)
    total = total.astype(low)
    for bit in reversed(places):
        other = swap(total, "dp", bit)
        high = upper("dp", bit)
        total = jnp.concatenate(
            [jnp.where(high, other, total), jnp.where(high, total, other)], axis=-2
        )
    return total.astype(wide)


def shards(
    inputs,
    out_grad,
    offsets,
    key_keep,
    project_weight,
    project_bias,
    output_weight,
    output_bias,
    norm_gains,
    norm_shifts,
    up_weight,
    up_bias,
    down_weight,
):
    width = inputs.shape[1]
    local_width = project_weight.shape[2]
    units = up_weight.shape[1]
    slot = lax.axis_index("tensor")
    ends = lax.dynamic_slice_in_dim(offsets, slot, 1)
    keep_row = lax.dynamic_slice_in_dim(key_keep, slot * SLOT, SLOT)
    position = jnp.arange(SLOT, dtype=jnp.int32)
    segment = (position >= ends[0, 0]).astype(jnp.int32) + (position >= ends[0, 1]).astype(
        jnp.int32
    )
    seg_start = (position == 0) | (position == ends[0, 0]) | (position == ends[0, 1])
    allowed = (segment[:, None] == segment[None, :]) & ((keep_row == 1) | seg_start)[None, :]
    live_mask = (segment < 2).astype(wide)[:, None]
    biases = output_bias.astype(wide)
    gains = norm_gains.astype(wide)
    shifts = norm_shifts.astype(wide)

    own_bias = jnp.concatenate([project_bias.reshape(-1), up_bias])
    lines = -(-own_bias.shape[0] // width)
    bias_rows = jnp.pad(own_bias, (0, 16 * width - own_bias.shape[0])).reshape(16, width)
    attn_block = jnp.concatenate(
        [project_weight.reshape(width, 3 * local_width).T, output_weight, bias_rows], axis=0
    )
    near, far = bits_of(lax.axis_size("tensor"))
    attn_near = swap(attn_block, "tensor", near)
    attn_far, _ = fetch_far(attn_block, ())
    up_far, (attn_far,) = fetch_far(up_weight, (attn_far,))
    attn_other = swap(attn_far, "dp", 1)
    up_near = swap(up_weight, "tensor", near)
    down_near = swap(down_weight, "tensor", near)
    attn_parts = [attn_block, attn_near]
    edge = 3 * local_width + output_weight.shape[0]
    count = 4

    def bias_of(part):
        return attn_parts[part][edge : edge + lines].reshape(-1)

    saved = []
    attended = 0.0
    for part in range(count):
        if part == 2:
            attended, attn_other = gate(attended, attn_other)
            attn_parts += spread(attn_far, attn_other)
        if part == 3:
            down_far, (up_far, attended) = fetch_far(down_weight, (up_far, attended))
            up_other = swap(up_far, "dp", 1)
        bias = bias_of(part).astype(wide)
        rows = matmul_nt(inputs, attn_parts[part][: 3 * local_width])
        query = (rows[:, :local_width] + bias[:local_width]).astype(low)
        keys = rows[:, local_width : 2 * local_width].astype(low)
        values = (rows[:, 2 * local_width :] + bias[local_width : 2 * local_width]).astype(low)
        context, log_total = attend(query, keys, values, allowed)
        attended = attended + matmul(context, attn_parts[part][3 * local_width : edge])
        saved.append((query, keys, values, context, log_total))

    up_other, down_far, attended = gate(up_other, down_far, attended)
    up_parts = [up_weight, up_near, *spread(up_far, up_other)]
    down_parts = [down_weight, down_near]
    down_other = swap(down_far, "dp", 1)
    resid_one = inputs.astype(wide) + attended + biases[0]
    unit_one, scale_one = norm_parts(resid_one)
    normed_one = unit_one * gains[0] + shifts[0]
    normed_low = normed_one.astype(low)
    ffn_out = 0.0
    kept = []
    for part in range(count):
        if part == 2:
            down_other, ffn_out = gate(down_other, ffn_out)
            down_parts += spread(down_far, down_other)
        bias = bias_of(part)[2 * local_width : 2 * local_width + units].astype(wide)
        active, slope = gelu_pair(matmul(normed_low, up_parts[part]) + bias)
        active = active.astype(low)
        ffn_out = ffn_out + matmul(active, down_parts[part])
        kept.append((active, slope))
    resid_two = normed_one + ffn_out + biases[1]
    unit_two, scale_two = norm_parts(resid_two)
    layer_output = ((unit_two * gains[1] + shifts[1]) * live_mask).astype(low)

    grad_out = out_grad.astype(wide) * live_mask
    grad_two, gain_two, shift_two = norm_back(unit_two, scale_two, gains[1], grad_out)
    grad_ffn = grad_two.astype(low)
    down_grads = [matmul_tn(kept[part][0], grad_ffn) for part in range(count)]
    down_three, down_one, grad_ffn = gate(
        down_grads[3].astype(low), down_grads[1].astype(low), grad_ffn
    )
    down_far_sum = near_sum(down_grads[2], down_three)
    down_total = near_sum(down_grads[0], down_one)
    grad_one_in = grad_two
    grad_pres = []
    for part in range(count):
        grad_act = matmul_nt(grad_ffn, down_parts[part])
        grad_pre = (grad_act * kept[part][1]).astype(low)
        grad_pres.append(grad_pre)
        grad_one_in = grad_one_in + matmul_nt(grad_pre, up_parts[part])
        if part == 1:
            down_far_low, grad_ffn, grad_one_in, down_total = gate(
                down_far_sum.astype(low), grad_ffn, grad_one_in, down_total
            )
            down_recv = swap(down_far_low, "tensor", far)
    up_grads = [matmul_tn(normed_low, grad_pres[part]) for part in range(count)]
    up_three, up_one, grad_one_in = gate(
        up_grads[3].astype(low), up_grads[1].astype(low), grad_one_in
    )
    up_far_low, grad_one_in = gate(
        near_sum(up_grads[2], up_three).astype(low), grad_one_in
    )
    up_recv = swap(up_far_low, "tensor", far)
    up_total = near_sum(up_grads[0], up_one)
    up_bias_grads = [jnp.sum(grad_pres[part], axis=0, dtype=wide) for part in range(count)]

    grad_one, gain_one, shift_one = norm_back(unit_one, scale_one, gains[0], grad_one_in)
    grad_attended = grad_one.astype(low)
    grad_input = 0.0
    extra = 8 * lax.axis_size("dp")
    attn_grads = {}
    shared = jnp.concatenate(
        [
            jnp.sum(grad_one, axis=0),
            jnp.sum(grad_two, axis=0),
            gain_one,
            gain_two,
            shift_one,
            shift_two,
        ]
    ).reshape(-1, width)
    for part in (3, 2, 1, 0):
        query, keys, values, context, log_total = saved[part]
        grad_context = matmul_nt(
            grad_attended, attn_parts[part][3 * local_width : edge]
        ).astype(low)
        pieces = attend_back(query, keys, values, grad_context, log_total, allowed)
        grad_rows = jnp.concatenate(pieces, axis=1)
        grad_input = grad_input + matmul(grad_rows, attn_parts[part][: 3 * local_width])
        own_small = jnp.concatenate(
            [
                jnp.sum(pieces[0], axis=0, dtype=wide),
                jnp.sum(pieces[2], axis=0, dtype=wide),
                up_bias_grads[part],
            ]
        )
        own_rows = jnp.pad(
            own_small, (0, (extra - shared.shape[0]) * width - own_small.shape[0])
        ).reshape(-1, width)
        attn_grads[part] = jnp.concatenate(
            [
                matmul_tn(grad_rows, inputs),
                matmul_tn(context, grad_attended),
                shared,
                own_rows,
            ],
            axis=0,
        )
        if part == 3:
            attn_three, down_recv, down_total, grad_attended = gate(
                attn_grads[3].astype(low), down_recv, down_total, grad_attended
            )
            down_total = halve(down_total + down_recv.astype(wide), 1)
        elif part == 2:
            attn_far_sum = near_sum(attn_grads[2], attn_three)
            attn_far_low, down_total, up_recv, up_total, grad_attended = gate(
                attn_far_sum.astype(low), down_total, up_recv, up_total, grad_attended
            )
            up_total = halve(up_total + up_recv.astype(wide), 1)
            down_total = halve(down_total, 2)
            attn_recv = swap(attn_far_low, "tensor", far)
        elif part == 1:
            attn_one, up_total, down_total, grad_attended = gate(
                attn_grads[1].astype(low), up_total, down_total, grad_attended
            )
            up_total = halve(up_total, 2)
    attn_total = near_sum(attn_grads[0], attn_one)
    attn_recv, grad_input, attn_total, up_total, down_total = gate(
        attn_recv, grad_input, attn_total, up_total, down_total
    )
    attn_total = attn_total + attn_recv.astype(wide)
    attn_grad = finish(attn_total, 0)
    up_weight_grad, down_weight_grad = finish(jnp.stack([up_total, down_total]), 2)
    input_grad = (grad_one + grad_input).astype(low)
    project_weight_grad = attn_grad[: 3 * local_width].T.reshape(width, 3, local_width)
    output_weight_grad = attn_grad[3 * local_width : edge]
    lower = edge + shared.shape[0]
    norm_grads = attn_grad[edge:lower].reshape(3, 2, width)
    own_small = attn_grad[lower : lower + lines].reshape(-1)
    project_bias_grad = own_small[: 2 * local_width].reshape(2, local_width)
    up_bias_grad = own_small[2 * local_width : 2 * local_width + units]
    return (
        layer_output,
        input_grad,
        project_weight_grad,
        project_bias_grad,
        output_weight_grad,
        norm_grads[0],
        norm_grads[1],
        norm_grads[2],
        up_weight_grad,
        up_bias_grad,
        down_weight_grad,
    )


def solution(mesh):
    in_specs = (
        P(("dp", "tensor"), None),
        P(("dp", "tensor"), None),
        P("dp", None),
        P("dp"),
        P(None, None, "tensor"),
        P(None, "tensor"),
        P("tensor", None),
        P(),
        P(),
        P(),
        P(None, "tensor"),
        P("tensor"),
        P("tensor", None),
    )
    out_specs = (
        P(("dp", "tensor"), None),
        P(("dp", "tensor"), None),
        P(None, None, "tensor"),
        P(None, "tensor"),
        P("tensor", None),
        P(),
        P(),
        P(),
        P(None, "tensor"),
        P("tensor"),
        P("tensor", None),
    )

    return jax.shard_map(shards, mesh=mesh, in_specs=in_specs, out_specs=out_specs, check_vma=False)
```

```python
import jax
import jax.numpy as jnp
from jax import lax
from jax.sharding import PartitionSpec as P


HD = 64
SLOT = 512

norm_epsilon = 1e-12
big_negative = -1e30
low = jnp.bfloat16
wide = jnp.float32


def bits_of(size):
    return [1 << place for place in range(size.bit_length() - 1)]


def swap(value, axis, bit):
    size = lax.axis_size(axis)
    return lax.ppermute(value, axis, [(index, index ^ bit) for index in range(size)])


def upper(axis, bit):
    return (lax.axis_index(axis) & bit) != 0


def norm_parts(resid):
    center = resid - jnp.mean(resid, axis=-1, keepdims=True)
    scale = lax.rsqrt(jnp.mean(center * center, axis=-1, keepdims=True) + norm_epsilon)
    return center * scale, scale


def norm_back(unit, scale, gain, grad):
    scaled = grad * gain
    back = scale * (
        scaled
        - jnp.mean(scaled, axis=-1, keepdims=True)
        - unit * jnp.mean(scaled * unit, axis=-1, keepdims=True)
    )
    return back, jnp.sum(grad * unit, axis=0), jnp.sum(grad, axis=0)


def gelu_pair(value):
    phi_sum = 0.5 * (1.0 + lax.erf(value * 0.7071067811865476))
    density = jnp.exp(-0.5 * value * value) * 0.3989422804014327
    return value * phi_sum, phi_sum + value * density


def matmul(left, right):
    return jnp.dot(left, right, preferred_element_type=wide)


def matmul_nt(left, right):
    return lax.dot_general(left, right, (((1,), (1,)), ((), ())), preferred_element_type=wide)


def matmul_tn(left, right):
    return lax.dot_general(left, right, (((0,), (0,)), ((), ())), preferred_element_type=wide)


def heads_of(rows):
    return rows.reshape(rows.shape[0], -1, HD)


def attend(query, keys, values, allowed):
    scores = jnp.einsum(
        "qhd,khd->hqk", heads_of(query), heads_of(keys), preferred_element_type=wide
    ) * HD ** (-0.5)
    scores = jnp.where(allowed[None], scores, big_negative)
    row_max = jnp.max(scores, axis=-1, keepdims=True)
    exponent = jnp.exp(scores - row_max)
    total = jnp.sum(exponent, axis=-1, keepdims=True)
    probs = (exponent / total).astype(low)
    context = jnp.einsum("hqk,khd->qhd", probs, heads_of(values), preferred_element_type=wide)
    return context.astype(low).reshape(query.shape), row_max + jnp.log(total)


def attend_back(query, keys, values, grad, log_total, allowed):
    scores = jnp.einsum(
        "qhd,khd->hqk", heads_of(query), heads_of(keys), preferred_element_type=wide
    ) * HD ** (-0.5)
    scores = jnp.where(allowed[None], scores, big_negative)
    probs = jnp.exp(scores - log_total)
    grad_heads = heads_of(grad)
    grad_probs = jnp.einsum(
        "qhd,khd->hqk", grad_heads, heads_of(values), preferred_element_type=wide
    )
    grad_value = jnp.einsum(
        "hqk,qhd->khd", probs.astype(low), grad_heads, preferred_element_type=wide
    )
    inner = jnp.sum(probs * grad_probs, axis=-1, keepdims=True)
    grad_scores = (probs * (grad_probs - inner)).astype(low)
    grad_query = jnp.einsum(
        "hqk,khd->qhd", grad_scores, heads_of(keys), preferred_element_type=wide
    ) * HD ** (-0.5)
    grad_key = jnp.einsum(
        "hqk,qhd->khd", grad_scores, heads_of(query), preferred_element_type=wide
    ) * HD ** (-0.5)
    return [part.astype(low).reshape(query.shape) for part in (grad_query, grad_key, grad_value)]


def gate(*values):
    return lax.optimization_barrier(values)


def fetch_far(block, after):
    far = bits_of(lax.axis_size("tensor"))[1]
    half = block.shape[0] // 2
    piece = lax.dynamic_slice_in_dim(block, jnp.where(upper("dp", 1), half, 0), half)
    piece, *after = gate(piece, *after)
    return swap(piece, "tensor", far), after


def spread(mine, other):
    high = upper("dp", 1)
    away = jnp.concatenate([jnp.where(high, other, mine), jnp.where(high, mine, other)], axis=0)
    return away, swap(away, "tensor", bits_of(lax.axis_size("tensor"))[0])


def near_sum(keep, send):
    near = bits_of(lax.axis_size("tensor"))[0]
    return keep + swap(send, "tensor", near).astype(wide)


def halve(total, bit):
    half = total.shape[0] // 2
    high = upper("dp", bit)
    keep = lax.dynamic_slice_in_dim(total, jnp.where(high, half, 0), half)
    send = lax.dynamic_slice_in_dim(total, jnp.where(high, 0, half), half)
    return keep + swap(send.astype(low), "dp", bit).astype(wide)


def finish(total, start):
    places = bits_of(lax.axis_size("dp"))
    for bit in places[start:]:
        total = halve(total, bit)
    total = total.astype(low)
    for bit in reversed(places):
        other = swap(total, "dp", bit)
        high = upper("dp", bit)
        total = jnp.concatenate(
            [jnp.where(high, other, total), jnp.where(high, total, other)], axis=0
        )
    return total.astype(wide)


def shards(
    inputs,
    out_grad,
    offsets,
    key_keep,
    project_weight,
    project_bias,
    output_weight,
    output_bias,
    norm_gains,
    norm_shifts,
    up_weight,
    up_bias,
    down_weight,
):
    width = inputs.shape[1]
    local_width = project_weight.shape[2]
    units = up_weight.shape[1]
    slot = lax.axis_index("tensor")
    ends = lax.dynamic_slice_in_dim(offsets, slot, 1)
    keep_row = lax.dynamic_slice_in_dim(key_keep, slot * SLOT, SLOT)
    position = jnp.arange(SLOT, dtype=jnp.int32)
    segment = (position >= ends[0, 0]).astype(jnp.int32) + (position >= ends[0, 1]).astype(
        jnp.int32
    )
    seg_start = (position == 0) | (position == ends[0, 0]) | (position == ends[0, 1])
    allowed = (segment[:, None] == segment[None, :]) & ((keep_row == 1) | seg_start)[None, :]
    live_mask = (segment < 2).astype(wide)[:, None]
    biases = output_bias.astype(wide)
    gains = norm_gains.astype(wide)
    shifts = norm_shifts.astype(wide)

    own_bias = jnp.concatenate([project_bias.reshape(-1), up_bias])
    lines = -(-own_bias.shape[0] // width)
    bias_rows = jnp.pad(own_bias, (0, 16 * width - own_bias.shape[0])).reshape(16, width)
    attn_block = jnp.concatenate(
        [project_weight.reshape(width, 3 * local_width).T, output_weight, bias_rows], axis=0
    )
    near, far = bits_of(lax.axis_size("tensor"))
    attn_near = swap(attn_block, "tensor", near)
    attn_far, _ = fetch_far(attn_block, ())
    up_far, (attn_far,) = fetch_far(up_weight, (attn_far,))
    attn_other = swap(attn_far, "dp", 1)
    up_near = swap(up_weight, "tensor", near)
    down_near = swap(down_weight, "tensor", near)
    attn_parts = [attn_block, attn_near]
    edge = 3 * local_width + output_weight.shape[0]
    count = 4

    def bias_of(part):
        return attn_parts[part][edge : edge + lines].reshape(-1)

    saved = []
    attended = 0.0
    for part in range(count):
        if part == 2:
            down_far, (up_far, attended, attn_other) = fetch_far(
                down_weight, (up_far, attended, attn_other)
            )
            attn_parts += spread(attn_far, attn_other)
            up_other = swap(up_far, "dp", 1)
        bias = bias_of(part).astype(wide)
        rows = matmul_nt(inputs, attn_parts[part][: 3 * local_width])
        query = (rows[:, :local_width] + bias[:local_width]).astype(low)
        keys = rows[:, local_width : 2 * local_width].astype(low)
        values = (rows[:, 2 * local_width :] + bias[local_width : 2 * local_width]).astype(low)
        context, log_total = attend(query, keys, values, allowed)
        attended = attended + matmul(context, attn_parts[part][3 * local_width : edge])
        saved.append((query, keys, values, context, log_total))

    up_other, down_far, attended = gate(up_other, down_far, attended)
    up_parts = [up_weight, up_near, *spread(up_far, up_other)]
    down_parts = [down_weight, down_near]
    down_other = swap(down_far, "dp", 1)
    resid_one = inputs.astype(wide) + attended + biases[0]
    unit_one, scale_one = norm_parts(resid_one)
    normed_one = unit_one * gains[0] + shifts[0]
    normed_low = normed_one.astype(low)
    ffn_out = 0.0
    kept = []
    for part in range(count):
        if part == 2:
            down_other, ffn_out = gate(down_other, ffn_out)
            down_parts += spread(down_far, down_other)
        bias = bias_of(part)[2 * local_width : 2 * local_width + units].astype(wide)
        active, slope = gelu_pair(matmul(normed_low, up_parts[part]) + bias)
        active = active.astype(low)
        ffn_out = ffn_out + matmul(active, down_parts[part])
        kept.append((active, slope))
    resid_two = normed_one + ffn_out + biases[1]
    unit_two, scale_two = norm_parts(resid_two)
    layer_output = ((unit_two * gains[1] + shifts[1]) * live_mask).astype(low)

    grad_out = out_grad.astype(wide) * live_mask
    grad_two, gain_two, shift_two = norm_back(unit_two, scale_two, gains[1], grad_out)
    grad_ffn = grad_two.astype(low)
    down_grads = [matmul_tn(kept[part][0], grad_ffn) for part in range(count)]
    down_three, down_one, grad_ffn = gate(
        down_grads[3].astype(low), down_grads[1].astype(low), grad_ffn
    )
    down_far_sum = near_sum(down_grads[2], down_three)
    down_total = near_sum(down_grads[0], down_one)
    grad_one_in = grad_two
    grad_pres = []
    for part in range(count):
        grad_act = matmul_nt(grad_ffn, down_parts[part])
        grad_pre = (grad_act * kept[part][1]).astype(low)
        grad_pres.append(grad_pre)
        grad_one_in = grad_one_in + matmul_nt(grad_pre, up_parts[part])
        if part == 1:
            down_far_low, grad_ffn, grad_one_in, down_total = gate(
                down_far_sum.astype(low), grad_ffn, grad_one_in, down_total
            )
            down_recv = swap(down_far_low, "tensor", far)
    up_grads = [matmul_tn(normed_low, grad_pres[part]) for part in range(count)]
    up_three, up_one, grad_one_in = gate(
        up_grads[3].astype(low), up_grads[1].astype(low), grad_one_in
    )
    up_far_low, grad_one_in = gate(
        near_sum(up_grads[2], up_three).astype(low), grad_one_in
    )
    up_recv = swap(up_far_low, "tensor", far)
    up_total = near_sum(up_grads[0], up_one)
    up_bias_grads = [jnp.sum(grad_pres[part], axis=0, dtype=wide) for part in range(count)]

    grad_one, gain_one, shift_one = norm_back(unit_one, scale_one, gains[0], grad_one_in)
    grad_attended = grad_one.astype(low)
    grad_input = 0.0
    extra = 8 * lax.axis_size("dp")
    attn_grads = {}
    shared = jnp.concatenate(
        [
            jnp.sum(grad_one, axis=0),
            jnp.sum(grad_two, axis=0),
            gain_one,
            gain_two,
            shift_one,
            shift_two,
        ]
    ).reshape(-1, width)
    for part in (3, 2, 1, 0):
        query, keys, values, context, log_total = saved[part]
        grad_context = matmul_nt(
            grad_attended, attn_parts[part][3 * local_width : edge]
        ).astype(low)
        pieces = attend_back(query, keys, values, grad_context, log_total, allowed)
        grad_rows = jnp.concatenate(pieces, axis=1)
        grad_input = grad_input + matmul(grad_rows, attn_parts[part][: 3 * local_width])
        own_small = jnp.concatenate(
            [
                jnp.sum(pieces[0], axis=0, dtype=wide),
                jnp.sum(pieces[2], axis=0, dtype=wide),
                up_bias_grads[part],
            ]
        )
        own_rows = jnp.pad(
            own_small, (0, (extra - shared.shape[0]) * width - own_small.shape[0])
        ).reshape(-1, width)
        attn_grads[part] = jnp.concatenate(
            [
                matmul_tn(grad_rows, inputs),
                matmul_tn(context, grad_attended),
                shared,
                own_rows,
            ],
            axis=0,
        )
        if part == 3:
            attn_three, down_recv, down_total, grad_attended = gate(
                attn_grads[3].astype(low), down_recv, down_total, grad_attended
            )
            down_total = halve(down_total + down_recv.astype(wide), 1)
        elif part == 2:
            attn_far_sum = near_sum(attn_grads[2], attn_three)
            attn_far_low, down_total, up_recv, up_total, grad_attended = gate(
                attn_far_sum.astype(low), down_total, up_recv, up_total, grad_attended
            )
            up_total = halve(up_total + up_recv.astype(wide), 1)
            attn_recv = swap(attn_far_low, "tensor", far)
        elif part == 1:
            attn_one, up_total, grad_attended = gate(
                attn_grads[1].astype(low), up_total, grad_attended
            )
    attn_total = near_sum(attn_grads[0], attn_one)
    attn_recv, grad_input, attn_total, up_total, down_total = gate(
        attn_recv, grad_input, attn_total, up_total, down_total
    )
    attn_total = attn_total + attn_recv.astype(wide)
    attn_grad = finish(attn_total, 0)
    up_weight_grad = finish(up_total, 1)
    down_weight_grad = finish(down_total, 1)
    input_grad = (grad_one + grad_input).astype(low)
    project_weight_grad = attn_grad[: 3 * local_width].T.reshape(width, 3, local_width)
    output_weight_grad = attn_grad[3 * local_width : edge]
    lower = edge + shared.shape[0]
    norm_grads = attn_grad[edge:lower].reshape(3, 2, width)
    own_small = attn_grad[lower : lower + lines].reshape(-1)
    project_bias_grad = own_small[: 2 * local_width].reshape(2, local_width)
    up_bias_grad = own_small[2 * local_width : 2 * local_width + units]
    return (
        layer_output,
        input_grad,
        project_weight_grad,
        project_bias_grad,
        output_weight_grad,
        norm_grads[0],
        norm_grads[1],
        norm_grads[2],
        up_weight_grad,
        up_bias_grad,
        down_weight_grad,
    )


def solution(mesh):
    in_specs = (
        P(("dp", "tensor"), None),
        P(("dp", "tensor"), None),
        P("dp", None),
        P("dp"),
        P(None, None, "tensor"),
        P(None, "tensor"),
        P("tensor", None),
        P(),
        P(),
        P(),
        P(None, "tensor"),
        P("tensor"),
        P("tensor", None),
    )
    out_specs = (
        P(("dp", "tensor"), None),
        P(("dp", "tensor"), None),
        P(None, None, "tensor"),
        P(None, "tensor"),
        P("tensor", None),
        P(),
        P(),
        P(),
        P(None, "tensor"),
        P("tensor"),
        P("tensor", None),
    )

    return jax.shard_map(shards, mesh=mesh, in_specs=in_specs, out_specs=out_specs, check_vma=False)
```

```python
import jax
import jax.numpy as jnp
from jax import lax
from jax.sharding import PartitionSpec as P


HD = 64
SLOT = 512

norm_epsilon = 1e-12
big_negative = -1e30
low = jnp.bfloat16
wide = jnp.float32


def bits_of(size):
    return [1 << place for place in range(size.bit_length() - 1)]


def swap(value, axis, bit):
    size = lax.axis_size(axis)
    return lax.ppermute(value, axis, [(index, index ^ bit) for index in range(size)])


def upper(axis, bit):
    return (lax.axis_index(axis) & bit) != 0


def norm_parts(resid):
    center = resid - jnp.mean(resid, axis=-1, keepdims=True)
    scale = lax.rsqrt(jnp.mean(center * center, axis=-1, keepdims=True) + norm_epsilon)
    return center * scale, scale


def norm_back(unit, scale, gain, grad):
    scaled = grad * gain
    back = scale * (
        scaled
        - jnp.mean(scaled, axis=-1, keepdims=True)
        - unit * jnp.mean(scaled * unit, axis=-1, keepdims=True)
    )
    return back, jnp.sum(grad * unit, axis=0), jnp.sum(grad, axis=0)


def gelu_pair(value):
    phi_sum = 0.5 * (1.0 + lax.erf(value * 0.7071067811865476))
    density = jnp.exp(-0.5 * value * value) * 0.3989422804014327
    return value * phi_sum, phi_sum + value * density


def matmul(left, right):
    return jnp.dot(left, right, preferred_element_type=wide)


def matmul_nt(left, right):
    return lax.dot_general(left, right, (((1,), (1,)), ((), ())), preferred_element_type=wide)


def matmul_tn(left, right):
    return lax.dot_general(left, right, (((0,), (0,)), ((), ())), preferred_element_type=wide)


def heads_of(rows):
    return rows.reshape(rows.shape[0], -1, HD)


def attend(query, keys, values, allowed):
    scores = jnp.einsum(
        "qhd,khd->hqk", heads_of(query), heads_of(keys), preferred_element_type=wide
    ) * HD ** (-0.5)
    scores = jnp.where(allowed[None], scores, big_negative)
    row_max = jnp.max(scores, axis=-1, keepdims=True)
    exponent = jnp.exp(scores - row_max)
    total = jnp.sum(exponent, axis=-1, keepdims=True)
    probs = (exponent / total).astype(low)
    context = jnp.einsum("hqk,khd->qhd", probs, heads_of(values), preferred_element_type=wide)
    return context.astype(low).reshape(query.shape), row_max + jnp.log(total)


def attend_back(query, keys, values, grad, log_total, allowed):
    scores = jnp.einsum(
        "qhd,khd->hqk", heads_of(query), heads_of(keys), preferred_element_type=wide
    ) * HD ** (-0.5)
    scores = jnp.where(allowed[None], scores, big_negative)
    probs = jnp.exp(scores - log_total)
    grad_heads = heads_of(grad)
    grad_probs = jnp.einsum(
        "qhd,khd->hqk", grad_heads, heads_of(values), preferred_element_type=wide
    )
    grad_value = jnp.einsum(
        "hqk,qhd->khd", probs.astype(low), grad_heads, preferred_element_type=wide
    )
    inner = jnp.sum(probs * grad_probs, axis=-1, keepdims=True)
    grad_scores = (probs * (grad_probs - inner)).astype(low)
    grad_query = jnp.einsum(
        "hqk,khd->qhd", grad_scores, heads_of(keys), preferred_element_type=wide
    ) * HD ** (-0.5)
    grad_key = jnp.einsum(
        "hqk,qhd->khd", grad_scores, heads_of(query), preferred_element_type=wide
    ) * HD ** (-0.5)
    return [part.astype(low).reshape(query.shape) for part in (grad_query, grad_key, grad_value)]


def gate(*values):
    return lax.optimization_barrier(values)


def fetch_far(block, after):
    far = bits_of(lax.axis_size("tensor"))[1]
    half = block.shape[0] // 2
    piece = lax.dynamic_slice_in_dim(block, jnp.where(upper("dp", 1), half, 0), half)
    piece, *after = gate(piece, *after)
    return swap(piece, "tensor", far), after


def spread(mine, other):
    high = upper("dp", 1)
    away = jnp.concatenate([jnp.where(high, other, mine), jnp.where(high, mine, other)], axis=0)
    return away, swap(away, "tensor", bits_of(lax.axis_size("tensor"))[0])


def near_sum(keep, send):
    near = bits_of(lax.axis_size("tensor"))[0]
    return keep + swap(send, "tensor", near).astype(wide)


def halve(total, bit):
    half = total.shape[0] // 2
    high = upper("dp", bit)
    keep = lax.dynamic_slice_in_dim(total, jnp.where(high, half, 0), half)
    send = lax.dynamic_slice_in_dim(total, jnp.where(high, 0, half), half)
    return keep + swap(send.astype(low), "dp", bit).astype(wide)


def finish(total, start):
    places = bits_of(lax.axis_size("dp"))
    for bit in places[start:]:
        total = halve(total, bit)
    total = total.astype(low)
    for bit in reversed(places):
        other = swap(total, "dp", bit)
        high = upper("dp", bit)
        total = jnp.concatenate(
            [jnp.where(high, other, total), jnp.where(high, total, other)], axis=0
        )
    return total.astype(wide)


def shards(
    inputs,
    out_grad,
    offsets,
    key_keep,
    project_weight,
    project_bias,
    output_weight,
    output_bias,
    norm_gains,
    norm_shifts,
    up_weight,
    up_bias,
    down_weight,
):
    width = inputs.shape[1]
    local_width = project_weight.shape[2]
    units = up_weight.shape[1]
    slot = lax.axis_index("tensor")
    ends = lax.dynamic_slice_in_dim(offsets, slot, 1)
    keep_row = lax.dynamic_slice_in_dim(key_keep, slot * SLOT, SLOT)
    position = jnp.arange(SLOT, dtype=jnp.int32)
    segment = (position >= ends[0, 0]).astype(jnp.int32) + (position >= ends[0, 1]).astype(
        jnp.int32
    )
    seg_start = (position == 0) | (position == ends[0, 0]) | (position == ends[0, 1])
    allowed = (segment[:, None] == segment[None, :]) & ((keep_row == 1) | seg_start)[None, :]
    live_mask = (segment < 2).astype(wide)[:, None]
    biases = output_bias.astype(wide)
    gains = norm_gains.astype(wide)
    shifts = norm_shifts.astype(wide)

    own_bias = jnp.concatenate([project_bias.reshape(-1), up_bias])
    lines = -(-own_bias.shape[0] // width)
    bias_rows = jnp.pad(own_bias, (0, 16 * width - own_bias.shape[0])).reshape(16, width)
    attn_block = jnp.concatenate(
        [project_weight.reshape(width, 3 * local_width).T, output_weight, bias_rows], axis=0
    )
    near, far = bits_of(lax.axis_size("tensor"))
    attn_near = swap(attn_block, "tensor", near)
    attn_far, _ = fetch_far(attn_block, ())
    up_far, (attn_far,) = fetch_far(up_weight, (attn_far,))
    attn_other = swap(attn_far, "dp", 1)
    up_near = swap(up_weight, "tensor", near)
    down_near = swap(down_weight, "tensor", near)
    attn_parts = [attn_block, attn_near]
    edge = 3 * local_width + output_weight.shape[0]
    count = 4

    def bias_of(part):
        return attn_parts[part][edge : edge + lines].reshape(-1)

    saved = []
    attended = 0.0
    for part in range(count):
        if part == 2:
            down_far, (up_far, attended, attn_other) = fetch_far(
                down_weight, (up_far, attended, attn_other)
            )
            attn_parts += spread(attn_far, attn_other)
            up_other = swap(up_far, "dp", 1)
        bias = bias_of(part).astype(wide)
        rows = matmul_nt(inputs, attn_parts[part][: 3 * local_width])
        query = (rows[:, :local_width] + bias[:local_width]).astype(low)
        keys = rows[:, local_width : 2 * local_width].astype(low)
        values = (rows[:, 2 * local_width :] + bias[local_width : 2 * local_width]).astype(low)
        context, log_total = attend(query, keys, values, allowed)
        attended = attended + matmul(context, attn_parts[part][3 * local_width : edge])
        saved.append((query, keys, values, context, log_total))

    up_other, down_far, attended = gate(up_other, down_far, attended)
    up_parts = [up_weight, up_near, *spread(up_far, up_other)]
    down_parts = [down_weight, down_near]
    down_other = swap(down_far, "dp", 1)
    resid_one = inputs.astype(wide) + attended + biases[0]
    unit_one, scale_one = norm_parts(resid_one)
    normed_one = unit_one * gains[0] + shifts[0]
    normed_low = normed_one.astype(low)
    ffn_out = 0.0
    kept = []
    for part in range(count):
        if part == 2:
            down_other, ffn_out = gate(down_other, ffn_out)
            down_parts += spread(down_far, down_other)
        bias = bias_of(part)[2 * local_width : 2 * local_width + units].astype(wide)
        active, slope = gelu_pair(matmul(normed_low, up_parts[part]) + bias)
        active = active.astype(low)
        ffn_out = ffn_out + matmul(active, down_parts[part])
        kept.append((active, slope))
    resid_two = normed_one + ffn_out + biases[1]
    unit_two, scale_two = norm_parts(resid_two)
    layer_output = ((unit_two * gains[1] + shifts[1]) * live_mask).astype(low)

    grad_out = out_grad.astype(wide) * live_mask
    grad_two, gain_two, shift_two = norm_back(unit_two, scale_two, gains[1], grad_out)
    grad_ffn = grad_two.astype(low)
    down_grads = [matmul_tn(kept[part][0], grad_ffn) for part in range(count)]
    down_three, down_one, grad_ffn = gate(
        down_grads[3].astype(low), down_grads[1].astype(low), grad_ffn
    )
    down_far_sum = near_sum(down_grads[2], down_three)
    down_total = near_sum(down_grads[0], down_one)
    grad_one_in = grad_two
    grad_pres = []
    for part in range(count):
        grad_act = matmul_nt(grad_ffn, down_parts[part])
        grad_pre = (grad_act * kept[part][1]).astype(low)
        grad_pres.append(grad_pre)
        grad_one_in = grad_one_in + matmul_nt(grad_pre, up_parts[part])
        if part == 1:
            down_far_low, grad_ffn, grad_one_in, down_total = gate(
                down_far_sum.astype(low), grad_ffn, grad_one_in, down_total
            )
            down_recv = swap(down_far_low, "tensor", far)
    up_grads = [matmul_tn(normed_low, grad_pres[part]) for part in range(count)]
    up_three, up_one, grad_one_in = gate(
        up_grads[3].astype(low), up_grads[1].astype(low), grad_one_in
    )
    up_far_low, grad_one_in = gate(
        near_sum(up_grads[2], up_three).astype(low), grad_one_in
    )
    up_recv = swap(up_far_low, "tensor", far)
    up_total = near_sum(up_grads[0], up_one)
    up_bias_grads = [jnp.sum(grad_pres[part], axis=0, dtype=wide) for part in range(count)]

    grad_one, gain_one, shift_one = norm_back(unit_one, scale_one, gains[0], grad_one_in)
    grad_attended = grad_one.astype(low)
    grad_input = 0.0
    extra = 8 * lax.axis_size("dp")
    attn_grads = {}
    shared = jnp.concatenate(
        [
            jnp.sum(grad_one, axis=0),
            jnp.sum(grad_two, axis=0),
            gain_one,
            gain_two,
            shift_one,
            shift_two,
        ]
    ).reshape(-1, width)
    for part in (3, 2, 1, 0):
        query, keys, values, context, log_total = saved[part]
        grad_context = matmul_nt(
            grad_attended, attn_parts[part][3 * local_width : edge]
        ).astype(low)
        pieces = attend_back(query, keys, values, grad_context, log_total, allowed)
        grad_rows = jnp.concatenate(pieces, axis=1)
        grad_input = grad_input + matmul(grad_rows, attn_parts[part][: 3 * local_width])
        own_small = jnp.concatenate(
            [
                jnp.sum(pieces[0], axis=0, dtype=wide),
                jnp.sum(pieces[2], axis=0, dtype=wide),
                up_bias_grads[part],
            ]
        )
        own_rows = jnp.pad(
            own_small, (0, (extra - shared.shape[0]) * width - own_small.shape[0])
        ).reshape(-1, width)
        attn_grads[part] = jnp.concatenate(
            [
                matmul_tn(grad_rows, inputs),
                matmul_tn(context, grad_attended),
                shared,
                own_rows,
            ],
            axis=0,
        )
        if part == 3:
            attn_three, down_recv, down_total, grad_attended = gate(
                attn_grads[3].astype(low), down_recv, down_total, grad_attended
            )
            down_total = halve(down_total + down_recv.astype(wide), 1)
        elif part == 2:
            attn_far_sum = near_sum(attn_grads[2], attn_three)
            attn_far_low, down_total, grad_attended = gate(
                attn_far_sum.astype(low), down_total, grad_attended
            )
            attn_recv = swap(attn_far_low, "tensor", far)
        elif part == 1:
            attn_one, up_recv, up_total, grad_attended = gate(
                attn_grads[1].astype(low), up_recv, up_total, grad_attended
            )
            up_total = halve(up_total + up_recv.astype(wide), 1)
    attn_total = near_sum(attn_grads[0], attn_one)
    attn_recv, grad_input, attn_total, up_total, down_total = gate(
        attn_recv, grad_input, attn_total, up_total, down_total
    )
    attn_total = attn_total + attn_recv.astype(wide)
    attn_grad = finish(attn_total, 0)
    up_weight_grad = finish(up_total, 1)
    down_weight_grad = finish(down_total, 1)
    input_grad = (grad_one + grad_input).astype(low)
    project_weight_grad = attn_grad[: 3 * local_width].T.reshape(width, 3, local_width)
    output_weight_grad = attn_grad[3 * local_width : edge]
    lower = edge + shared.shape[0]
    norm_grads = attn_grad[edge:lower].reshape(3, 2, width)
    own_small = attn_grad[lower : lower + lines].reshape(-1)
    project_bias_grad = own_small[: 2 * local_width].reshape(2, local_width)
    up_bias_grad = own_small[2 * local_width : 2 * local_width + units]
    return (
        layer_output,
        input_grad,
        project_weight_grad,
        project_bias_grad,
        output_weight_grad,
        norm_grads[0],
        norm_grads[1],
        norm_grads[2],
        up_weight_grad,
        up_bias_grad,
        down_weight_grad,
    )


def solution(mesh):
    in_specs = (
        P(("dp", "tensor"), None),
        P(("dp", "tensor"), None),
        P("dp", None),
        P("dp"),
        P(None, None, "tensor"),
        P(None, "tensor"),
        P("tensor", None),
        P(),
        P(),
        P(),
        P(None, "tensor"),
        P("tensor"),
        P("tensor", None),
    )
    out_specs = (
        P(("dp", "tensor"), None),
        P(("dp", "tensor"), None),
        P(None, None, "tensor"),
        P(None, "tensor"),
        P("tensor", None),
        P(),
        P(),
        P(),
        P(None, "tensor"),
        P("tensor"),
        P("tensor", None),
    )

    return jax.shard_map(shards, mesh=mesh, in_specs=in_specs, out_specs=out_specs, check_vma=False)
```
